32 devices in a mesh: ma: 8 (over z, y), pb: 4 (over x, core).
Axes of the slice: x: 2, y: 2, z: 4, core: 2. Of those that a mesh axis runs over, the one named last changes fastest.
Arguments:
- coefs: float32 [512, 1056, 64], P('ma', 'pb'), may hold values from -6 to 6
- legendre: float32 [512, 1056, 4, 256], P('ma', None, 'pb'), may hold values from -0.25 to 0.25
- quad_weight: float32 [4, 256], P('pb'), may hold values from 0.3 to 3
- pair_of_slot: int32 [512], replicated, may hold values from 0 to 511, each once
- tracers: float32 [12, 2, 1024, 2048], P(None, None, ('ma', 'pb')), may hold values from 0 to 2
- heat_rate: float32 [12, 2], replicated, may hold values from -1.75 to 1.75
Outputs:
- spec_tendency: float32 [512, 1056, 64], P('ma', 'pb')
- tracers_new: float32 [12, 2, 1024, 2048], P(None, None, ('ma', 'pb'))
The draws below stay inside these ranges and needn't reach their ends.
Inputs may be any that keep to these rules, and one draw needn't show every extreme that they name: Each pair number appears once; slot s holds the orders pair_of_slot[s] and 1023 - pair_of_slot[s].
All inputs are finite; a program needn't handle non-finite values.
Results may differ from the reference program's by a relative error of at most 0.00007.
Values sent between devices are 32-bit elements; how exact they have to be, the bound alone decides.
A program may use at most 320 MiB of HBM per device.

```python
import math
import jax
import jax.numpy as jnp
from jax import lax

M = 1024
NLAT = 1024
NLON = 2048
LAYER_TOTAL = 8
NF = 4
NTR = 12
TLEV = 2
PAIRS = 512
PROWS = 1056
COLS = 64
QLAT = 256
BAND = 32
N_MA = 8
N_PB = 4


def steps_of(rng, dims, shards, low, largest):
    loudness = 1.0
    for dim, shards_of in shards:
        heights = jax.random.uniform(jax.random.fold_in(jax.random.fold_in(rng, 6), dim), (shards_of,), jnp.float32, low / len(shards), largest / len(shards))
        loudness = loudness * jnp.repeat(jnp.exp(heights), dims[dim] // shards_of).reshape((-1,) + (1,) * (len(dims) - 1 - dim))
    return loudness


def scatter_about(rng, extent, spread, most, shards=(), held_as=jnp.bfloat16):
    array = spread * jax.random.normal(rng, extent, jnp.float32)
    if shards:
        array = array * steps_of(rng, extent, shards, -0.22, 0.18)
    return jnp.clip(array, -most, most).astype(held_as)


def setup_inputs(seed: int = 0) -> dict:
    arg_keys = jax.random.split(jax.random.key(seed), 7)
    return {
        "coefs": scatter_about(arg_keys[0], (PAIRS, PROWS, COLS), 1.0, 6.0, ((0, 8), (1, 4)), jnp.float32),
        "legendre": scatter_about(arg_keys[1], (PAIRS, PROWS, N_PB, QLAT), (M // 2) ** -0.5, 0.25, ((0, 8), (2, 4)), jnp.float32),
        "quad_weight": jnp.clip(jnp.exp(math.log(3.0) - 2.3025851 * jax.random.uniform(arg_keys[2], (N_PB, QLAT), jnp.float32) ** steps_of(arg_keys[2], (N_PB, QLAT), ((0, 4),), -0.2, 0.2)), 0.3, 3.0),
        "pair_of_slot": jax.random.permutation(arg_keys[3], PAIRS).astype(jnp.int32),
        "tracers": jnp.clip(2.0 * jax.random.uniform(arg_keys[4], (NTR, TLEV, NLAT, NLON), jnp.float32) ** steps_of(arg_keys[4], (NTR, TLEV, NLAT, NLON), ((2, 32),), -0.2, 0.2), 0.0, 2.0),
        "heat_rate": scatter_about(arg_keys[5], (NTR, TLEV), NTR ** -0.5, 1.75, (), jnp.float32),
    }


COURANT = 0.15
DRAG_COEFFICIENT = 0.2
MOISTURE_SOURCE = 0.3
RAINFALL_FACTOR = 0.2
HIGHEST = lax.Precision.HIGHEST

def order_tables(pair_of_slot):
    lowest = pair_of_slot.astype(jnp.int32)
    orders = jnp.stack([lowest, M - 1 - lowest], axis=1)
    points = jnp.arange(NLON, dtype=jnp.int32)
    phases = orders[:, :, None] * points[None, None, :] % NLON
    angles = phases.astype(jnp.float32) * (2.0 * math.pi / NLON)
    factor = 1.0 / math.sqrt(NLON)
    fourier_table = jnp.stack([jnp.cos(angles) * factor, -jnp.sin(angles) * factor], axis=0)
    weights = jnp.where(orders == 0, 1.0, 2.0).astype(jnp.float32)
    return (fourier_table, weights)

def row_masks(pair_ids, row_start, row_count):
    row_ids = row_start + jnp.arange(row_count, dtype=jnp.int32)
    bounds = (M - pair_ids.astype(jnp.int32))[:, None]
    low_rows = row_ids[None, :] < bounds
    high_rows = (row_ids[None, :] >= bounds) & (row_ids[None, :] <= M)
    return (low_rows, high_rows)

def advect(padded, zonal_wind, southward, first_row):
    middle = padded[:, :, 1:-1, :]
    east_face = 0.5 * (zonal_wind + jnp.roll(zonal_wind, -1, axis=-1))
    flux_east = jnp.maximum(east_face, 0.0) * middle + jnp.minimum(east_face, 0.0) * jnp.roll(middle, -1, axis=-1)
    across = 0.5 * (southward[:, :-1, :] + southward[:, 1:, :])
    flux_south = jnp.maximum(across, 0.0) * padded[:, :, :-1, :] + jnp.minimum(across, 0.0) * padded[:, :, 1:, :]
    upper_row = first_row - 1 + jnp.arange(across.shape[1], dtype=jnp.int32)
    inside = (upper_row >= 0) & (upper_row <= NLAT - 2)
    flux_south = jnp.where(inside[None, None, :, None], flux_south, 0.0)
    change = flux_east - jnp.roll(flux_east, 1, axis=-1) + (flux_south[:, :, 1:, :] - flux_south[:, :, :-1, :])
    return -COURANT * change

def reference(coefs, legendre, quad_weight, pair_of_slot, tracers, heat_rate):
    legendre_rows = legendre.reshape(PAIRS, PROWS, NLAT)
    low_rows, high_rows = row_masks(pair_of_slot, 0, PROWS)
    masked = jnp.concatenate([jnp.where(low_rows[:, :, None], coefs, 0.0), jnp.where(high_rows[:, :, None], coefs, 0.0)], axis=2)
    stored = jnp.einsum('srl,src->slc', legendre_rows, masked, precision=HIGHEST)
    latitudes = stored.reshape(PAIRS, N_PB, N_MA, BAND, 2 * COLS).transpose(0, 2, 1, 3, 4).reshape(PAIRS, NLAT, 2 * COLS)
    fourier_table, weights = order_tables(pair_of_slot)
    spectral = latitudes.reshape(PAIRS, NLAT, 2, 2, NF * LAYER_TOTAL) * weights[:, None, :, None, None]
    physical_space_field = jnp.einsum('sjhpc,pshi->jci', spectral, fourier_table, precision=HIGHEST)
    zonal_wind = jnp.transpose(physical_space_field[:, 0:TLEV, :], (1, 0, 2))
    southward = -jnp.transpose(physical_space_field[:, LAYER_TOTAL:LAYER_TOTAL + TLEV, :], (1, 0, 2))
    southward_ext = jnp.pad(southward, ((0, 0), (1, 1), (0, 0)))

    def runge_section(tracer_field):
        padded = jnp.pad(tracer_field, ((0, 0), (0, 0), (1, 1), (0, 0)))
        return advect(padded, zonal_wind, southward_ext, 0)
    first_section = tracers + runge_section(tracers)
    second = 0.75 * tracers + 0.25 * (first_section + runge_section(first_section))
    tracers_new = tracers / 3.0 + 2.0 / 3.0 * (second + runge_section(second))
    heating = jnp.einsum('kl,klji->jli', heat_rate, tracers_new, precision=HIGHEST)
    eastward_finished = physical_space_field[:, 0:LAYER_TOTAL]
    northward_velocity = physical_space_field[:, LAYER_TOTAL:2 * LAYER_TOTAL]
    thermal_state = physical_space_field[:, 2 * LAYER_TOTAL:3 * LAYER_TOTAL]
    vapour_mixing_share = physical_space_field[:, 3 * LAYER_TOTAL:4 * LAYER_TOTAL]
    flow_speed_norm = jnp.sqrt(eastward_finished * eastward_finished + northward_velocity * northward_velocity + 1.0)
    warming_finished = jnp.pad(heating, ((0, 0), (0, LAYER_TOTAL - TLEV), (0, 0)))
    rate_of_change_field = jnp.concatenate([-DRAG_COEFFICIENT * flow_speed_norm * eastward_finished, -DRAG_COEFFICIENT * flow_speed_norm * northward_velocity, warming_finished - MOISTURE_SOURCE * thermal_state * vapour_mixing_share, MOISTURE_SOURCE * thermal_state * vapour_mixing_share - RAINFALL_FACTOR * flow_speed_norm * vapour_mixing_share], axis=1)
    fourier = jnp.einsum('jci,pshi->sjhpc', rate_of_change_field, fourier_table, precision=HIGHEST).reshape(PAIRS, NLAT, 2 * COLS)
    stored_back = fourier.reshape(PAIRS, N_MA, N_PB, BAND, 2 * COLS).transpose(0, 2, 1, 3, 4).reshape(PAIRS, NLAT, 2 * COLS)
    weighted = stored_back * quad_weight.reshape(NLAT)[None, :, None]
    row_sums = jnp.einsum('srl,slc->src', legendre_rows, weighted, precision=HIGHEST)
    spec_tendency = jnp.where(low_rows[:, :, None], row_sums[:, :, :COLS], 0.0) + jnp.where(high_rows[:, :, None], row_sums[:, :, COLS:], 0.0)
    return (spec_tendency, tracers_new)
```

```python
import math

import jax
import jax.numpy as jnp
from jax import lax
from jax.experimental import pallas as pl
from jax.experimental.pallas import tpu as pltpu
from jax.sharding import PartitionSpec as P

M = 1024
NLAT = 1024
NLON = 2048
LAYER_TOTAL = 8
NF = 4
NTR = 12
TLEV = 2
PAIRS = 512


COURANT = 0.15
DRAG_COEFFICIENT = 0.2
MOISTURE_SOURCE = 0.3
RAINFALL_FACTOR = 0.2
HIGH = lax.Precision.HIGH

HALO = 3
EDGE = 8


def halo_rows(block, axes, dim, width):
    count = lax.axis_size(axes)
    forward = [(i, i + 1) for i in range(count - 1)]
    backward = [(target, source) for source, target in forward]
    low = lax.ppermute(
        lax.slice_in_dim(block, block.shape[dim] - width, None, axis=dim), axes, forward
    )
    high = lax.ppermute(lax.slice_in_dim(block, 0, width, axis=dim), axes, backward)
    return low, high


def split_orders(pair_ids):
    low_even = pair_ids % 2 == 0
    even = jnp.where(low_even, pair_ids, M - 1 - pair_ids)
    return low_even, even, M - 1 - even


def half_tables(orders, points):
    step = 128
    coarse_ids = jnp.arange(points // step, dtype=jnp.int32) * step
    fine_ids = jnp.arange(step, dtype=jnp.int32)
    unit = 2.0 * math.pi / NLON
    coarse = (orders[:, None] * coarse_ids[None, :] % NLON).astype(jnp.float32) * unit
    fine = (orders[:, None] * fine_ids[None, :] % NLON).astype(jnp.float32) * unit
    factor = 1.0 / math.sqrt(NLON)
    cc, sc = lax.optimization_barrier((jnp.cos(coarse) * factor, jnp.sin(coarse) * factor))
    cf, sf = lax.optimization_barrier((jnp.cos(fine), jnp.sin(fine)))
    cos = [cc[:, a : a + 1] * cf - sc[:, a : a + 1] * sf for a in range(points // step)]
    sin = [-(sc[:, a : a + 1] * cf + cc[:, a : a + 1] * sf) for a in range(points // step)]
    return jnp.stack([jnp.concatenate(cos, axis=1), jnp.concatenate(sin, axis=1)], axis=0)


def transport_kernel(
    first_ref, rate_ref, q_ref, ql_ref, qh_ref, u_ref, ul_ref, uh_ref, w_ref, wl_ref, wh_ref,
    out_ref, heat_ref, pad, ap, an, bp, bn,
):
    rows = q_ref.shape[2]
    total = rows + 2 * EDGE
    lons = q_ref.shape[3]
    level = pl.program_id(0)
    tracer = pl.program_id(1)

    def fill(mid, low, high):
        pad[EDGE : EDGE + rows, :] = mid
        pad[EDGE - HALO : EDGE, :] = low
        pad[EDGE + rows : EDGE + rows + HALO, :] = high

    @pl.when(tracer == 0)
    def _():
        fill(u_ref[0], ul_ref[0], uh_ref[0])
        u = pad[...]
        face = (0.5 * COURANT) * (u + pltpu.roll(u, lons - 1, 1))
        ap[...] = jnp.maximum(face, 0.0)
        an[...] = jnp.minimum(face, 0.0)
        fill(w_ref[0], wl_ref[0], wh_ref[0])
        w = pad[...]
        face = (-0.5 * COURANT) * (w + pltpu.roll(w, total - 1, 0))
        upper = first_ref[0] - EDGE + lax.broadcasted_iota(jnp.int32, (total, lons), 0)
        inside = (upper >= 0) & (upper <= NLAT - 2)
        bp[...] = jnp.where(inside, jnp.maximum(face, 0.0), 0.0)
        bn[...] = jnp.where(inside, jnp.minimum(face, 0.0), 0.0)

    def step(q):
        east = ap[...] * q + an[...] * pltpu.roll(q, lons - 1, 1)
        south = bp[...] * q + bn[...] * pltpu.roll(q, total - 1, 0)
        return q - ((east - pltpu.roll(east, 1, 1)) + (south - pltpu.roll(south, 1, 0)))

    fill(q_ref[0, 0], ql_ref[0, 0], qh_ref[0, 0])
    q = pad[...]
    second = 0.75 * q + 0.25 * step(step(q))
    third = step(second)[EDGE : EDGE + rows]
    new = q_ref[0, 0] * (1.0 / 3.0) + (2.0 / 3.0) * third
    out_ref[0, 0] = new
    warm = rate_ref[tracer, level] * new

    @pl.when(tracer == 0)
    def _():
        heat_ref[0] = warm

    @pl.when(tracer > 0)
    def _():
        heat_ref[0] += warm


def transport(first_row, heat_rate, tracers, low, high, wind, wind_low, wind_high):
    count, levels, rows, lons = tracers.shape
    total = rows + 2 * EDGE

    def tracer_spec(height):
        return pl.BlockSpec((1, 1, height, lons), lambda l, k: (k, l, 0, 0))

    def wind_spec(height):
        return pl.BlockSpec((1, height, lons), lambda l, k: (l, 0, 0))

    smem = pl.BlockSpec(memory_space=pltpu.SMEM)
    return pl.pallas_call(
        transport_kernel,
        grid=(levels, count),
        in_specs=[smem, smem]
        + [tracer_spec(rows), tracer_spec(HALO), tracer_spec(HALO)]
        + [wind_spec(rows), wind_spec(HALO), wind_spec(HALO)] * 2,
        out_specs=[tracer_spec(rows), wind_spec(rows)],
        out_shape=[
            jax.ShapeDtypeStruct(tracers.shape, tracers.dtype),
            jax.ShapeDtypeStruct((levels, rows, lons), tracers.dtype),
        ],
        scratch_shapes=[pltpu.VMEM((total, lons), jnp.float32)] * 5,
        compiler_params=pltpu.CompilerParams(
            dimension_semantics=("arbitrary", "arbitrary"), vmem_limit_bytes=40 * 1024 * 1024
        ),
    )(
        first_row.reshape(1), heat_rate, tracers, low, high,
        wind[0], wind_low[0], wind_high[0], wind[1], wind_low[1], wind_high[1],
    )


MESH = pl.DeviceIdType.MESH
GROUP = 8
RING = 4


def partner(index, count, step):
    if step == 1:
        return index + 1 - 2 * (index % 2)
    if step == 2:
        return (index + count // 2) % count
    return count - 1 - index


def split(x):
    high = x.astype(jnp.bfloat16)
    return high, (x - high.astype(jnp.float32)).astype(jnp.bfloat16)


def product(left, right, contract):
    dims = ((contract[:1], contract[1:]), ((), ()))
    rows = left.shape[0]
    left_high, left_low = split(left)
    right_high, right_low = split(right)
    both = lax.dot_general(
        jnp.concatenate([left_high, left_low], axis=0), right_high, dims,
        preferred_element_type=jnp.float32,
    )
    rest = lax.dot_general(left_high, right_low, dims, preferred_element_type=jnp.float32)
    return both[:rows] + (both[rows:] + rest)


def rows_of(ref, start, count):
    return jnp.concatenate(
        [ref[pl.ds(2 * start, count, 2), :], ref[pl.ds(2 * start + 1, count, 2), :]], axis=1
    )


def order_rows(pair_ref, slot, first, count):
    pair = pair_ref[slot]
    bound = M - pair
    low_even = pair % 2 == 0
    even_from, even_to = jnp.where(low_even, 0, bound), jnp.where(low_even, bound, M + 1)
    odd_from, odd_to = jnp.where(low_even, bound, 0), jnp.where(low_even, M + 1, bound)
    rows = first + lax.broadcasted_iota(jnp.int32, (1, count), 1)
    even = (rows >= even_from) & (rows < even_to)
    odd = (rows >= odd_from) & (rows < odd_to)
    return even, odd, jnp.where(pair == 0, 1.0, 2.0)


def enter(band_count, here, quarter_count, quarter):
    barrier = pltpu.get_barrier_semaphore()
    for step in range(1, band_count):
        pl.semaphore_signal(
            barrier, inc=1, device_id={"ma": (here + step) % band_count}, device_id_type=MESH
        )
    for step in (1, 2):
        pl.semaphore_signal(
            barrier, inc=1, device_id={"pb": partner(quarter, quarter_count, step)},
            device_id_type=MESH,
        )
    pl.semaphore_wait(barrier, band_count + 1)


def stream_rows(legendre_ref, held, sem, slot):
    return pltpu.make_async_copy(legendre_ref.at[slot], held.at[slot % RING], sem.at[slot % RING])


def analysis_kernel(
    pair_ref, coefs_ref, legendre_ref, out_ref,
    pieces, held, sums, load_sem, own_sem, near_send, near_recv, far_send, far_recv,
    pass_send, pass_recv, send_sem, recv_sem, keep_sem,
):
    slots, columns, piece = coefs_ref.shape
    chunks = slots // GROUP
    count = lax.axis_size("ma")
    here = lax.axis_index("ma")
    quarters = lax.axis_size("pb")
    quarter = lax.axis_index("pb")
    near, far = partner(quarter, quarters, 1), partner(quarter, quarters, 2)
    band = sums.shape[1] // count
    width = sums.shape[1] // GROUP
    weight_columns = 2 * columns

    def part(ref, chunk):
        return ref.at[pl.ds(chunk * GROUP, GROUP)]

    def own(chunk):
        return pltpu.make_async_copy(
            part(coefs_ref, chunk), part(pieces.at[0], chunk), own_sem.at[chunk]
        )

    def to_near(chunk):
        return pltpu.make_async_remote_copy(
            part(coefs_ref, chunk), part(pieces.at[1], chunk),
            near_send.at[chunk], near_recv.at[chunk],
            device_id={"pb": near}, device_id_type=MESH,
        )

    def to_far(chunk):
        return pltpu.make_async_remote_copy(
            part(coefs_ref, chunk), part(pieces.at[2], chunk),
            far_send.at[chunk], far_recv.at[chunk],
            device_id={"pb": far}, device_id_type=MESH,
        )

    def pass_on(chunk):
        return pltpu.make_async_remote_copy(
            part(pieces.at[2], chunk), part(pieces.at[3], chunk),
            pass_send.at[chunk], pass_recv.at[chunk],
            device_id={"pb": near}, device_id_type=MESH,
        )

    def to_band(chunk, step):
        target = (here + step) % count
        return pltpu.make_async_remote_copy(
            sums.at[chunk, pl.ds(target * band, band)], out_ref.at[here, chunk],
            send_sem.at[step - 1, chunk], recv_sem.at[step - 1, chunk],
            device_id={"ma": target}, device_id_type=MESH,
        )

    def keep(chunk):
        return pltpu.make_async_copy(
            sums.at[chunk, pl.ds(here * band, band)], out_ref.at[here, chunk], keep_sem.at[chunk]
        )

    for slot in range(RING - 1):
        stream_rows(legendre_ref, held, load_sem, slot).start()
    enter(count, here, quarters, quarter)

    def begin(chunk, carry):
        to_far(chunk).start()
        to_near(chunk).start()
        own(chunk).start()
        return carry

    lax.fori_loop(0, chunks, begin, 0)

    def one_slot(slot, chunk):
        stream_rows(legendre_ref, held, load_sem, slot).wait()

        @pl.when(slot + RING - 1 < slots)
        def _():
            stream_rows(legendre_ref, held, load_sem, slot + RING - 1).start()

        block = held.at[slot % RING]
        total = jnp.zeros((weight_columns, width), jnp.float32)
        for k in range(quarters):
            first = (quarter if k == 0 else partner(quarter, quarters, k)) * piece
            even, odd, even_weight = order_rows(pair_ref, slot, first, piece)
            x = pieces[k, slot]
            both = jnp.concatenate(
                [jnp.where(even, x * even_weight, 0.0), jnp.where(odd, x * 2.0, 0.0)], axis=0
            )
            total = total + product(both, rows_of(block, first, piece), (1, 0))
        sums[chunk, pl.ds(slot % GROUP, width, GROUP), :] = total.T

    def one_chunk(chunk, carry):
        to_far(chunk).wait_recv()
        pass_on(chunk).start()
        own(chunk).wait()
        to_near(chunk).wait_recv()
        pass_on(chunk).wait_recv()

        def body(i, inner):
            one_slot(chunk * GROUP + i, chunk)
            return inner

        lax.fori_loop(0, GROUP, body, 0)
        keep(chunk).start()
        for step in range(1, count):
            to_band(chunk, step).start()
        return carry

    lax.fori_loop(0, chunks, one_chunk, 0)

    def finish(chunk, carry):
        to_far(chunk).wait_send()
        to_near(chunk).wait_send()
        pass_on(chunk).wait_send()
        keep(chunk).wait()
        for step in range(1, count):
            to_band(chunk, step).wait()
        return carry

    lax.fori_loop(0, chunks, finish, 0)


def analysis(pairs, coefs, legendre, band_count):
    slots, columns, piece = coefs.shape
    chunks = slots // GROUP
    half_rows, lanes = legendre.shape[1:]
    quarters = half_rows // (2 * piece)
    width = 2 * lanes
    band = width // band_count
    any_space = pl.BlockSpec(memory_space=pl.ANY)
    dma = pltpu.SemaphoreType.DMA
    return pl.pallas_call(
        analysis_kernel,
        in_specs=[pl.BlockSpec(memory_space=pltpu.SMEM), any_space, any_space],
        out_specs=any_space,
        out_shape=jax.ShapeDtypeStruct(
            (band_count, chunks, band * GROUP, 2 * columns), jnp.float32
        ),
        scratch_shapes=[
            pltpu.VMEM((quarters, slots, columns, piece), jnp.float32),
            pltpu.VMEM((RING, half_rows, lanes), jnp.float32),
            pltpu.VMEM((chunks, width * GROUP, 2 * columns), jnp.float32),
            dma((RING,)),
        ]
        + [dma((chunks,))] * 7
        + [dma((band_count - 1, chunks))] * 2
        + [dma((chunks,))],
        compiler_params=pltpu.CompilerParams(
            collective_id=0, has_side_effects=True, vmem_limit_bytes=60 * 1024 * 1024
        ),
    )(pairs, coefs, legendre)


def synthesis_kernel(
    pair_ref, quad_ref, fourier_ref, legendre_ref, out_ref,
    bands, held, parts, near_held, far_held, load_sem, send_sem, recv_sem, keep_sem,
    near_send, near_recv, far_send, far_recv, out_sem,
):
    slots, columns, piece = out_ref.shape
    chunks = slots // GROUP
    count = lax.axis_size("ma")
    here = lax.axis_index("ma")
    quarters = lax.axis_size("pb")
    quarter = lax.axis_index("pb")
    near, far = partner(quarter, quarters, 1), partner(quarter, quarters, 2)
    band = bands.shape[1] // count
    width = bands.shape[1] // GROUP

    def to_orders(chunk, step):
        target = (here + step) % count
        return pltpu.make_async_remote_copy(
            fourier_ref.at[target, chunk], bands.at[chunk, pl.ds(here * band, band)],
            send_sem.at[step - 1, chunk], recv_sem.at[step - 1, chunk],
            device_id={"ma": target}, device_id_type=MESH,
        )

    def keep(chunk):
        return pltpu.make_async_copy(
            fourier_ref.at[here, chunk], bands.at[chunk, pl.ds(here * band, band)],
            keep_sem.at[chunk],
        )

    def to_near(chunk, k):
        return pltpu.make_async_remote_copy(
            parts.at[chunk, 2 * k + 1], near_held.at[chunk, k],
            near_send.at[k, chunk], near_recv.at[k, chunk],
            device_id={"pb": near}, device_id_type=MESH,
        )

    def to_far(chunk):
        return pltpu.make_async_remote_copy(
            parts.at[chunk, 2], far_held.at[chunk], far_send.at[chunk], far_recv.at[chunk],
            device_id={"pb": far}, device_id_type=MESH,
        )

    def store(chunk):
        return pltpu.make_async_copy(
            parts.at[chunk, 0], out_ref.at[pl.ds(chunk * GROUP, GROUP)], out_sem.at[chunk]
        )

    for slot in range(RING - 1):
        stream_rows(legendre_ref, held, load_sem, slot).start()
    enter(count, here, quarters, quarter)

    def begin(chunk, carry):
        for step in range(1, count):
            to_orders(chunk, step).start()
        keep(chunk).start()
        return carry

    lax.fori_loop(0, chunks, begin, 0)

    def one_slot(slot, chunk):
        stream_rows(legendre_ref, held, load_sem, slot).wait()

        @pl.when(slot + RING - 1 < slots)
        def _():
            stream_rows(legendre_ref, held, load_sem, slot + RING - 1).start()

        block = held.at[slot % RING]
        own = slot % GROUP
        weighted = bands[chunk, pl.ds(own, width, GROUP), :].T * quad_ref[...]
        for k in range(quarters):
            first = (quarter if k == 0 else partner(quarter, quarters, k)) * piece
            even, odd, _ = order_rows(pair_ref, slot, first, piece)
            both = product(weighted, rows_of(block, first, piece), (1, 1))
            parts[chunk, k, own] = jnp.where(
                even, both[:columns], jnp.where(odd, both[columns:], 0.0)
            )

    def complete(chunk):
        to_far(chunk).wait_recv()

        def body(i, carry):
            parts[chunk, 0, i] = parts[chunk, 0, i] + near_held[chunk, 0, i] + far_held[chunk, i]
            return carry

        lax.fori_loop(0, GROUP, body, 0)
        store(chunk).start()

    def one_chunk(chunk, carry):
        keep(chunk).wait()
        for step in range(1, count):
            to_orders(chunk, step).wait_recv()

        def body(i, inner):
            one_slot(chunk * GROUP + i, chunk)
            return inner

        lax.fori_loop(0, GROUP, body, 0)
        to_near(chunk, 1).start()
        to_near(chunk, 0).start()

        @pl.when(chunk > 0)
        def _():
            complete(chunk - 1)

        to_near(chunk, 1).wait_recv()

        def add(i, inner):
            parts[chunk, 2, i] = parts[chunk, 2, i] + near_held[chunk, 1, i]
            return inner

        lax.fori_loop(0, GROUP, add, 0)
        to_near(chunk, 0).wait_recv()
        to_far(chunk).start()
        return carry

    lax.fori_loop(0, chunks, one_chunk, 0)
    complete(chunks - 1)

    def finish(chunk, carry):
        for step in range(1, count):
            to_orders(chunk, step).wait_send()
        to_near(chunk, 0).wait_send()
        to_near(chunk, 1).wait_send()
        to_far(chunk).wait_send()
        store(chunk).wait()
        return carry

    lax.fori_loop(0, chunks, finish, 0)


def synthesis(pairs, quad, fourier, legendre, piece):
    band_count, chunks, rows, columns = fourier.shape
    slots = chunks * GROUP
    columns = columns // 2
    half_rows, lanes = legendre.shape[1:]
    quarters = half_rows // (2 * piece)
    any_space = pl.BlockSpec(memory_space=pl.ANY)
    dma = pltpu.SemaphoreType.DMA
    block = (GROUP, columns, piece)
    return pl.pallas_call(
        synthesis_kernel,
        in_specs=[
            pl.BlockSpec(memory_space=pltpu.SMEM), pl.BlockSpec(memory_space=pltpu.VMEM),
            any_space, any_space,
        ],
        out_specs=any_space,
        out_shape=jax.ShapeDtypeStruct((slots, columns, piece), jnp.float32),
        scratch_shapes=[
            pltpu.VMEM((chunks, band_count * rows, 2 * columns), jnp.float32),
            pltpu.VMEM((RING, half_rows, lanes), jnp.float32),
            pltpu.VMEM((chunks, quarters) + block, jnp.float32),
            pltpu.VMEM((chunks, 2) + block, jnp.float32),
            pltpu.VMEM((chunks,) + block, jnp.float32),
            dma((RING,)),
            dma((band_count - 1, chunks)),
            dma((band_count - 1, chunks)),
            dma((chunks,)),
            dma((2, chunks)),
            dma((2, chunks)),
            dma((chunks,)),
            dma((chunks,)),
            dma((chunks,)),
        ],
        compiler_params=pltpu.CompilerParams(
            collective_id=1, has_side_effects=True, vmem_limit_bytes=63 * 1024 * 1024
        ),
    )(pairs, quad, fourier, legendre)


LATS = 8


def to_grid_kernel(spectral_ref, high_ref, low_ref, out_ref, left):
    sources, chunks = spectral_ref.shape[:2]
    slots = sources * chunks * GROUP
    part = NF * LAYER_TOTAL
    half = high_ref.shape[2]

    for j in range(LATS):
        block = spectral_ref[:, :, j * GROUP : (j + 1) * GROUP, :].reshape(slots, 4 * part).T
        for h in range(2):
            for p in range(2):
                left[h, j * part : (j + 1) * part, p * slots : (p + 1) * slots] = block[
                    (2 * h + p) * part : (2 * h + p + 1) * part
                ]
    sums = []
    for h in range(2):
        high, low = split(left[h])
        dot = lambda a, b: jnp.dot(a, b, preferred_element_type=jnp.float32)
        sums.append(dot(high, high_ref[h]) + (dot(low, high_ref[h]) + dot(high, low_ref[h])))
    out_ref[:, :half] = sums[0] + sums[1]
    out_ref[:, half:] = sums[0] - sums[1]


def to_grid(spectral, high, low):
    sources, chunks, rows, lanes = spectral.shape
    part = NF * LAYER_TOTAL
    lats = rows // GROUP
    tables = pl.BlockSpec(high.shape, lambda j: (0, 0, 0))
    return pl.pallas_call(
        to_grid_kernel,
        grid=(lats // LATS,),
        in_specs=[
            pl.BlockSpec((sources, chunks, LATS * GROUP, lanes), lambda j: (0, 0, j, 0)),
            tables,
            tables,
        ],
        out_specs=pl.BlockSpec((LATS * part, NLON), lambda j: (j, 0)),
        out_shape=jax.ShapeDtypeStruct((lats * part, NLON), jnp.float32),
        scratch_shapes=[pltpu.VMEM((2, LATS * part, high.shape[1]), jnp.float32)],
        compiler_params=pltpu.CompilerParams(vmem_limit_bytes=60 * 1024 * 1024),
    )(spectral, high, low)


def from_grid_kernel(field_ref, heat_ref, high_ref, low_ref, out_ref, left, turned):
    sources, chunks = out_ref.shape[:2]
    slots = sources * chunks * GROUP
    part = NF * LAYER_TOTAL
    half = high_ref.shape[2]
    lev = LAYER_TOTAL

    for j in range(LATS):
        def tendency(cols):
            at = lambda f: field_ref[j * part + f * lev : j * part + (f + 1) * lev, cols]
            u, v, t, q = at(0), at(1), at(2), at(3)
            speed = jnp.sqrt(u * u + v * v + 1.0)
            moist = MOISTURE_SOURCE * t * q
            return jnp.concatenate(
                [
                    -DRAG_COEFFICIENT * speed * u,
                    -DRAG_COEFFICIENT * speed * v,
                    heat_ref[j, :, cols] - moist,
                    moist - RAINFALL_FACTOR * speed * q,
                ],
                axis=0,
            )

        near = tendency(slice(0, half))
        far = tendency(slice(half, 2 * half))
        left[0, j * part : (j + 1) * part] = near + far
        left[1, j * part : (j + 1) * part] = near - far
    dims = (((1,), (1,)), ((), ()))
    for h in range(2):
        high, low = split(left[h])
        dot = lambda a, b: lax.dot_general(a, b, dims, preferred_element_type=jnp.float32)
        both = dot(high, high_ref[h]) + (dot(low, high_ref[h]) + dot(high, low_ref[h]))
        for j in range(LATS):
            for p in range(2):
                turned[j, (2 * h + p) * part : (2 * h + p + 1) * part] = both[
                    j * part : (j + 1) * part, p * slots : (p + 1) * slots
                ]
    for j in range(LATS):
        out_ref[:, :, j * GROUP : (j + 1) * GROUP, :] = turned[j].T.reshape(
            sources, chunks, GROUP, 4 * part
        )


def from_grid(field, heat, high, low, sources, chunks):
    part = NF * LAYER_TOTAL
    lats = field.shape[0] // part
    slots = sources * chunks * GROUP
    tables = pl.BlockSpec(high.shape, lambda j: (0, 0, 0))
    return pl.pallas_call(
        from_grid_kernel,
        grid=(lats // LATS,),
        in_specs=[
            pl.BlockSpec((LATS * part, NLON), lambda j: (j, 0)),
            pl.BlockSpec((LATS, LAYER_TOTAL, NLON), lambda j: (j, 0, 0)),
            tables,
            tables,
        ],
        out_specs=pl.BlockSpec(
            (sources, chunks, LATS * GROUP, 4 * part), lambda j: (0, 0, j, 0)
        ),
        out_shape=jax.ShapeDtypeStruct((sources, chunks, lats * GROUP, 4 * part), jnp.float32),
        scratch_shapes=[
            pltpu.VMEM((2, LATS * part, high.shape[2]), jnp.float32),
            pltpu.VMEM((LATS, 4 * part, slots), jnp.float32),
        ],
        compiler_params=pltpu.CompilerParams(vmem_limit_bytes=60 * 1024 * 1024),
    )(field, heat, high, low)


def fourier_tables(pair_of_slot):
    _, even_all, odd_all = split_orders(pair_of_slot)
    half = NLON // 2
    tables = jnp.stack([half_tables(even_all, half), half_tables(odd_all, half)], axis=0)
    tables = tables.reshape(2, -1, half)
    high = lax.reduce_precision(tables, 8, 7)
    return high.astype(jnp.bfloat16), (tables - high).astype(jnp.bfloat16)


def shards(coefs, legendre, quad_weight, pair_of_slot, tracers, heat_rate):
    slot_count, piece = coefs.shape[:2]
    quarter = legendre.shape[3]
    part = NF * LAYER_TOTAL
    band_count = lax.axis_size("ma")
    lanes = 128
    legendre_rows = legendre.reshape(slot_count, -1, lanes)
    own_pairs = lax.dynamic_slice_in_dim(
        pair_of_slot, lax.axis_index("ma") * slot_count, slot_count, 0
    )
    low, high = halo_rows(tracers, ("ma", "pb"), 2, HALO)
    table_high, table_low = fourier_tables(pair_of_slot)
    spectral = analysis(own_pairs, jnp.transpose(coefs, (0, 2, 1)), legendre_rows, band_count)
    field = to_grid(spectral, table_high, table_low)
    band_rows = field.shape[0] // part
    grid = field.reshape(band_rows, part, NLON)
    wind = jnp.stack(
        [
            jnp.transpose(grid[:, 0:TLEV, :], (1, 0, 2)),
            jnp.transpose(grid[:, LAYER_TOTAL : LAYER_TOTAL + TLEV, :], (1, 0, 2)),
        ],
        axis=0,
    )
    wind_low, wind_high = halo_rows(wind, ("ma", "pb"), 2, HALO)
    first_row = (lax.axis_index(("ma", "pb")) * band_rows).astype(jnp.int32)
    new_tracers, heating = transport(
        first_row, heat_rate, tracers, low, high, wind, wind_low, wind_high
    )
    heating = jnp.transpose(heating, (1, 0, 2))
    warming = jnp.pad(heating, ((0, 0), (0, LAYER_TOTAL - TLEV), (0, 0)))
    fourier = from_grid(
        field, warming, table_high, table_low, band_count, slot_count // GROUP
    )
    spec = synthesis(own_pairs, quad_weight.reshape(1, quarter), fourier, legendre_rows, piece)
    return (jnp.transpose(spec, (0, 2, 1)), new_tracers)


def solution(mesh):
    in_specs = (
        P("ma", "pb", None),
        P("ma", None, "pb", None),
        P("pb", None),
        P(),
        P(None, None, ("ma", "pb"), None),
        P(),
    )
    out_specs = (P("ma", "pb", None), P(None, None, ("ma", "pb"), None))
    return jax.shard_map(shards, mesh=mesh, in_specs=in_specs, out_specs=out_specs, check_vma=False)
```

```python
import math

import jax
import jax.numpy as jnp
from jax import lax
from jax.experimental import pallas as pl
from jax.experimental.pallas import tpu as pltpu
from jax.sharding import PartitionSpec as P

M = 1024
NLAT = 1024
NLON = 2048
LAYER_TOTAL = 8
NF = 4
NTR = 12
TLEV = 2
PAIRS = 512


COURANT = 0.15
DRAG_COEFFICIENT = 0.2
MOISTURE_SOURCE = 0.3
RAINFALL_FACTOR = 0.2
HIGH = lax.Precision.HIGH

HALO = 3
EDGE = 8


def split_orders(pair_ids):
    low_even = pair_ids % 2 == 0
    even = jnp.where(low_even, pair_ids, M - 1 - pair_ids)
    return low_even, even, M - 1 - even


def half_tables(orders, points):
    step = 128
    coarse_ids = jnp.arange(points // step, dtype=jnp.int32) * step
    fine_ids = jnp.arange(step, dtype=jnp.int32)
    unit = 2.0 * math.pi / NLON
    coarse = (orders[:, None] * coarse_ids[None, :] % NLON).astype(jnp.float32) * unit
    fine = (orders[:, None] * fine_ids[None, :] % NLON).astype(jnp.float32) * unit
    factor = 1.0 / math.sqrt(NLON)
    cc, sc = lax.optimization_barrier((jnp.cos(coarse) * factor, jnp.sin(coarse) * factor))
    cf, sf = lax.optimization_barrier((jnp.cos(fine), jnp.sin(fine)))
    cos = [cc[:, a : a + 1] * cf - sc[:, a : a + 1] * sf for a in range(points // step)]
    sin = [-(sc[:, a : a + 1] * cf + cc[:, a : a + 1] * sf) for a in range(points // step)]
    return jnp.stack([jnp.concatenate(cos, axis=1), jnp.concatenate(sin, axis=1)], axis=0)


MESH = pl.DeviceIdType.MESH
GROUP = 8
RING = 4
LATS = 8
UNIT = 2
PART = NF * LAYER_TOTAL


def partner(index, count, step):
    if step == 1:
        return index + 1 - 2 * (index % 2)
    if step == 2:
        return (index + count // 2) % count
    return count - 1 - index


def split(x):
    high = x.astype(jnp.bfloat16)
    return high, (x - high.astype(jnp.float32)).astype(jnp.bfloat16)


def product(left, right, contract):
    dims = ((contract[:1], contract[1:]), ((), ()))
    rows = left.shape[0]
    left_high, left_low = split(left)
    right_high, right_low = split(right)
    both = lax.dot_general(
        jnp.concatenate([left_high, left_low], axis=0), right_high, dims,
        preferred_element_type=jnp.float32,
    )
    rest = lax.dot_general(left_high, right_low, dims, preferred_element_type=jnp.float32)
    return both[:rows] + (both[rows:] + rest)


def rows_of(ref, start, count):
    return jnp.concatenate(
        [ref[pl.ds(2 * start, count, 2), :], ref[pl.ds(2 * start + 1, count, 2), :]], axis=1
    )


def order_rows(pair_ref, slot, first, count):
    pair = pair_ref[slot]
    bound = M - pair
    low_even = pair % 2 == 0
    even_from, even_to = jnp.where(low_even, 0, bound), jnp.where(low_even, bound, M + 1)
    odd_from, odd_to = jnp.where(low_even, bound, 0), jnp.where(low_even, M + 1, bound)
    rows = first + lax.broadcasted_iota(jnp.int32, (1, count), 1)
    even = (rows >= even_from) & (rows < even_to)
    odd = (rows >= odd_from) & (rows < odd_to)
    return even, odd, jnp.where(pair == 0, 1.0, 2.0)


def fourier_tables(pair_of_slot):
    _, even_all, odd_all = split_orders(pair_of_slot)
    half = NLON // 2
    tables = jnp.stack([half_tables(even_all, half), half_tables(odd_all, half)], axis=0)
    tables = tables.reshape(2, -1, half)
    high = lax.reduce_precision(tables, 8, 7)
    return high.astype(jnp.bfloat16), (tables - high).astype(jnp.bfloat16)


def transport_kernel(
    first_ref, rate_ref, q_ref, ql_ref, qh_ref, u_ref, ul_ref, uh_ref, w_ref, wl_ref, wh_ref,
    out_ref, heat_ref, pad, ap, an, bp, bn,
):
    rows = q_ref.shape[2]
    total = rows + EDGE
    lons = q_ref.shape[3]
    level = pl.program_id(0)
    tracer = pl.program_id(1)
    edge_rows = lax.broadcasted_iota(jnp.int32, (EDGE, lons), 0)

    @pl.when(tracer == 0)
    def _():
        pad[0:EDGE, :] = jnp.where(edge_rows < EDGE // 2, uh_ref[0], ul_ref[0])
        pad[EDGE:total, :] = u_ref[0]
        u = pad[...]
        face = (0.5 * COURANT) * (u + pltpu.roll(u, lons - 1, 1))
        ap[...] = jnp.maximum(face, 0.0)
        an[...] = jnp.minimum(face, 0.0)
        pad[0:EDGE, :] = jnp.where(edge_rows < EDGE // 2, wh_ref[0], wl_ref[0])
        pad[EDGE:total, :] = w_ref[0]
        w = pad[...]
        face = (-0.5 * COURANT) * (w + pltpu.roll(w, total - 1, 0))
        place = lax.broadcasted_iota(jnp.int32, (total, lons), 0)
        upper = first_ref[0] + jnp.where(place < EDGE // 2, rows + place, place - EDGE)
        inside = (upper >= 0) & (upper <= NLAT - 2)
        bp[...] = jnp.where(inside, jnp.maximum(face, 0.0), 0.0)
        bn[...] = jnp.where(inside, jnp.minimum(face, 0.0), 0.0)
        pad[0:EDGE, :] = jnp.zeros((EDGE, lons), jnp.float32)

    def step(q):
        east = ap[...] * q + an[...] * pltpu.roll(q, lons - 1, 1)
        south = bp[...] * q + bn[...] * pltpu.roll(q, total - 1, 0)
        return q - ((east - pltpu.roll(east, 1, 1)) + (south - pltpu.roll(south, 1, 0)))

    pad[0:HALO, :] = qh_ref[0, 0]
    pad[EDGE - HALO : EDGE, :] = ql_ref[0, 0]
    pad[EDGE:total, :] = q_ref[0, 0]
    q = pad[...]
    second = 0.75 * q + 0.25 * step(step(q))
    third = step(second)[EDGE:total]
    new = q_ref[0, 0] * (1.0 / 3.0) + (2.0 / 3.0) * third
    out_ref[0, 0] = new
    warm = rate_ref[tracer, level] * new

    @pl.when(tracer == 0)
    def _():
        heat_ref[0] = warm

    @pl.when(tracer > 0)
    def _():
        heat_ref[0] += warm


def transport(first_row, heat_rate, tracers, low, high, wind, wind_low, wind_high):
    count, levels, rows, lons = tracers.shape
    total = rows + EDGE

    def tracer_spec(height):
        return pl.BlockSpec((1, 1, height, lons), lambda l, k: (k, l, 0, 0))

    def wind_spec(height, first):
        return pl.BlockSpec((1, height, lons), lambda l, k: (l + first, 0, 0))

    smem = pl.BlockSpec(memory_space=pltpu.SMEM)
    return pl.pallas_call(
        transport_kernel,
        grid=(levels, count),
        in_specs=[smem, smem]
        + [tracer_spec(rows), tracer_spec(HALO), tracer_spec(HALO)]
        + [wind_spec(rows, 0), wind_spec(EDGE, 0), wind_spec(EDGE, 0)]
        + [wind_spec(rows, levels), wind_spec(EDGE, levels), wind_spec(EDGE, levels)],
        out_specs=[tracer_spec(rows), wind_spec(rows, 0)],
        out_shape=[
            jax.ShapeDtypeStruct(tracers.shape, tracers.dtype),
            jax.ShapeDtypeStruct((levels, rows, lons), tracers.dtype),
        ],
        scratch_shapes=[pltpu.VMEM((total, lons), jnp.float32)] * 5,
        compiler_params=pltpu.CompilerParams(
            dimension_semantics=("arbitrary", "arbitrary"), vmem_limit_bytes=40 * 1024 * 1024
        ),
    )(
        first_row.reshape(1), heat_rate, tracers, low, high,
        wind, wind_low, wind_high, wind, wind_low, wind_high,
    )


def neighbour(band, count, quarter, quarters, step):
    place = (band * quarters + quarter + step + count * quarters) % (count * quarters)
    return {"ma": place // quarters, "pb": place % quarters}


def enter(band_count, here, quarter_count, quarter, beside):
    barrier = pltpu.get_barrier_semaphore()
    others = [{"ma": (here + step) % band_count} for step in range(1, band_count)]
    others += [{"pb": partner(quarter, quarter_count, step)} for step in (1, 2)]
    for other in others + beside:
        pl.semaphore_signal(barrier, inc=1, device_id=other, device_id_type=MESH)
    pl.semaphore_wait(barrier, len(others) + len(beside))


def stream_rows(legendre_ref, held, sem, slot):
    return pltpu.make_async_copy(legendre_ref.at[slot], held.at[slot % RING], sem.at[slot % RING])


def wait_bytes(ref, sem):
    pltpu.make_async_copy(ref, ref, sem).wait()


def to_grid(spectral_ref, high_ref, low_ref, out_ref, left):
    sources, chunks = spectral_ref.shape[:2]
    slots = sources * chunks * GROUP
    half = high_ref.shape[2]
    for j in range(LATS):
        block = spectral_ref[:, :, j * GROUP : (j + 1) * GROUP, :].reshape(slots, 4 * PART).T
        for h in range(2):
            for p in range(2):
                left[h, j * PART : (j + 1) * PART, p * slots : (p + 1) * slots] = block[
                    (2 * h + p) * PART : (2 * h + p + 1) * PART
                ]
    sums = []
    for h in range(2):
        high, low = split(left[h])
        dot = lambda a, b: jnp.dot(a, b, preferred_element_type=jnp.float32)
        sums.append(dot(high, high_ref[h]) + (dot(low, high_ref[h]) + dot(high, low_ref[h])))
    out_ref[:, :half] = sums[0] + sums[1]
    out_ref[:, half:] = sums[0] - sums[1]


def from_grid(field_ref, heat_ref, first, high_ref, low_ref, out_ref, left, turned):
    sources, chunks = out_ref.shape[:2]
    slots = sources * chunks * GROUP
    half = high_ref.shape[2]
    lev = LAYER_TOTAL
    level = lax.broadcasted_iota(jnp.int32, (lev, half), 0)

    for j in range(LATS):
        def tendency(start):
            cols = slice(start, start + half)
            at = lambda f: field_ref[j * PART + f * lev : j * PART + (f + 1) * lev, cols]
            u, v, t, q = at(0), at(1), at(2), at(3)
            speed = jnp.sqrt(u * u + v * v + 1.0)
            moist = MOISTURE_SOURCE * t * q
            warm = jnp.zeros((lev, half), jnp.float32)
            for l in range(TLEV):
                rows = heat_ref[l, pl.ds(first, LATS), cols]
                warm = jnp.where(level == l, rows[j : j + 1], warm)
            return jnp.concatenate(
                [
                    -DRAG_COEFFICIENT * speed * u,
                    -DRAG_COEFFICIENT * speed * v,
                    warm - moist,
                    moist - RAINFALL_FACTOR * speed * q,
                ],
                axis=0,
            )

        near = tendency(0)
        far = tendency(half)
        left[0, j * PART : (j + 1) * PART] = near + far
        left[1, j * PART : (j + 1) * PART] = near - far
    dims = (((1,), (1,)), ((), ()))
    for h in range(2):
        high, low = split(left[h])
        dot = lambda a, b: lax.dot_general(a, b, dims, preferred_element_type=jnp.float32)
        both = dot(high, high_ref[h]) + (dot(low, high_ref[h]) + dot(high, low_ref[h]))
        for j in range(LATS):
            for p in range(2):
                turned[j, (2 * h + p) * PART : (2 * h + p + 1) * PART] = both[
                    j * PART : (j + 1) * PART, p * slots : (p + 1) * slots
                ]
    for j in range(LATS):
        out_ref[:, :, j * GROUP : (j + 1) * GROUP, :] = turned[j].T.reshape(
            sources, chunks, GROUP, 4 * PART
        )


def analysis_kernel(
    pair_ref, coefs_ref, legendre_ref, high_ref, low_ref, above_ref, below_ref,
    field_ref, wind_ref, wind_low_ref, wind_high_ref, trace_low_ref, trace_high_ref, bands_ref,
    pieces, held, sums, high, low, block, left, field, wind,
    load_sem, own_sem, near_send, near_recv, far_send, far_recv,
    pass_send, pass_recv, send_sem, recv_sem, keep_sem, table_sem, trace_send, trace_recv,
    block_sem, field_sem, wind_sem, edge_send, edge_recv,
):
    slots, columns, piece = coefs_ref.shape
    chunks = slots // GROUP
    count = lax.axis_size("ma")
    here = lax.axis_index("ma")
    quarters = lax.axis_size("pb")
    quarter = lax.axis_index("pb")
    near, far = partner(quarter, quarters, 1), partner(quarter, quarters, 2)
    after = neighbour(here, count, quarter, quarters, 1)
    before = neighbour(here, count, quarter, quarters, -1)
    band = sums.shape[1] // count
    width = sums.shape[1] // GROUP
    weight_columns = 2 * columns
    groups = band // (LATS * GROUP)
    late = LATS * GROUP
    early = band - late
    spans = ((0, early), (early, late))

    def part(ref, chunk):
        return ref.at[pl.ds(chunk * GROUP, GROUP)]

    def remote(source, target, sends, receives, device):
        return pltpu.make_async_remote_copy(
            source, target, sends, receives, device_id=device, device_id_type=MESH
        )

    def own(chunk):
        return pltpu.make_async_copy(
            part(coefs_ref, chunk), part(pieces.at[0], chunk), own_sem.at[chunk]
        )

    def to_near(chunk):
        return remote(
            part(coefs_ref, chunk), part(pieces.at[1], chunk),
            near_send.at[chunk], near_recv.at[chunk], {"pb": near},
        )

    def to_far(chunk):
        return remote(
            part(coefs_ref, chunk), part(pieces.at[2], chunk),
            far_send.at[chunk], far_recv.at[chunk], {"pb": far},
        )

    def pass_on(chunk):
        return remote(
            part(pieces.at[2], chunk), part(pieces.at[3], chunk),
            pass_send.at[chunk], pass_recv.at[chunk], {"pb": near},
        )

    def send_bands(chunk, which):
        start, size = spans[which]
        for step in range(1, count):
            target = (here + step) % count
            remote(
                sums.at[chunk, pl.ds(target * band + start, size)],
                bands_ref.at[here, chunk, pl.ds(start, size)],
                send_sem.at[which], recv_sem.at[which], {"ma": target},
            ).start()
        pltpu.make_async_copy(
            sums.at[chunk, pl.ds(here * band + start, size)],
            bands_ref.at[here, chunk, pl.ds(start, size)],
            keep_sem.at[which],
        ).start()

    def wait_bands(which):
        start, size = spans[which]
        wait_bytes(bands_ref.at[pl.ds(0, count - 1), :, pl.ds(start, size)], recv_sem.at[which])
        wait_bytes(bands_ref.at[0, :, pl.ds(start, size)], keep_sem.at[which])

    tables = [
        pltpu.make_async_copy(high_ref, high, table_sem.at[0]),
        pltpu.make_async_copy(low_ref, low, table_sem.at[1]),
    ]
    traces = [
        remote(above_ref, trace_high_ref, trace_send.at[0], trace_recv.at[0], before),
        remote(below_ref, trace_low_ref, trace_send.at[1], trace_recv.at[1], after),
    ]

    for slot in range(RING - 1):
        stream_rows(legendre_ref, held, load_sem, slot).start()
    enter(count, here, quarters, quarter, [after, before])

    def begin(chunk, carry):
        to_far(chunk).start()
        to_near(chunk).start()
        own(chunk).start()
        return carry

    lax.fori_loop(0, chunks, begin, 0)

    def one_slot(slot, chunk):
        stream_rows(legendre_ref, held, load_sem, slot).wait()

        @pl.when(slot + RING - 1 < slots)
        def _():
            stream_rows(legendre_ref, held, load_sem, slot + RING - 1).start()

        rows = held.at[slot % RING]
        total = jnp.zeros((weight_columns, width), jnp.float32)
        for k in range(quarters):
            first = (quarter if k == 0 else partner(quarter, quarters, k)) * piece
            even, odd, even_weight = order_rows(pair_ref, slot, first, piece)
            x = pieces[k, slot]
            both = jnp.concatenate(
                [jnp.where(even, x * even_weight, 0.0), jnp.where(odd, x * 2.0, 0.0)], axis=0
            )
            total = total + product(both, rows_of(rows, first, piece), (1, 0))
        sums[chunk, pl.ds(slot % GROUP, width, GROUP), :] = total.T

    def one_chunk(chunk, carry):
        to_far(chunk).wait_recv()
        pass_on(chunk).start()
        own(chunk).wait()
        to_near(chunk).wait_recv()
        pass_on(chunk).wait_recv()

        def body(i, inner):
            one_slot(chunk * GROUP + i, chunk)
            return inner

        lax.fori_loop(0, GROUP, body, 0)
        if early:
            send_bands(chunk, 0)
        return carry

    lax.fori_loop(0, chunks, one_chunk, 0)

    def send_late(chunk, carry):
        send_bands(chunk, 1)
        return carry

    lax.fori_loop(0, chunks, send_late, 0)
    for copy in tables + traces:
        copy.start()

    def load(group):
        return pltpu.make_async_copy(
            bands_ref.at[:, :, pl.ds(group * late, late)], block.at[group % 2],
            block_sem.at[group % 2],
        )

    def store(group):
        return pltpu.make_async_copy(
            field.at[group % 2], field_ref.at[pl.ds(group * LATS * PART, LATS * PART)],
            field_sem.at[group % 2],
        )

    for copy in tables:
        copy.wait()
    wait_bands(0 if early else 1)
    load(0).start()

    def one_group(group, carry):
        load(group).wait()

        @pl.when(group + 2 < groups)
        def _():
            load(group + 1).start()

        @pl.when(group + 2 == groups)
        def _():
            wait_bands(1)
            load(group + 1).start()

        @pl.when(group >= 2)
        def _():
            store(group - 2).wait()

        to_grid(block.at[group % 2], high, low, field.at[group % 2], left)
        store(group).start()
        for component in range(2):
            for l in range(TLEV):
                row = component * LAYER_TOTAL + l
                wind[component * TLEV + l, pl.ds(group * LATS, LATS), :] = jnp.concatenate(
                    [
                        field[group % 2, j * PART + row : j * PART + row + 1, :]
                        for j in range(LATS)
                    ],
                    axis=0,
                )
        return carry

    lax.fori_loop(0, groups, one_group, 0)
    lats = groups * LATS
    edges = [
        remote(
            wind.at[:, pl.ds(0, EDGE)], wind_high_ref, edge_send.at[0], edge_recv.at[0], before
        ),
        remote(
            wind.at[:, pl.ds(lats - EDGE, EDGE)], wind_low_ref,
            edge_send.at[1], edge_recv.at[1], after,
        ),
    ]
    winds = pltpu.make_async_copy(wind, wind_ref, wind_sem)
    for copy in edges + [winds]:
        copy.start()

    def finish(chunk, carry):
        to_far(chunk).wait_send()
        to_near(chunk).wait_send()
        pass_on(chunk).wait_send()
        return carry

    lax.fori_loop(0, chunks, finish, 0)
    for which in range(0 if early else 1, 2):
        start, size = spans[which]
        wait_bytes(bands_ref.at[pl.ds(0, count - 1), :, pl.ds(start, size)], send_sem.at[which])
    for group in range(max(groups - 2, 0), groups):
        store(group).wait()
    for copy in traces + edges + [winds]:
        copy.wait()


def analysis(pairs, coefs, legendre, high, low, above, below, band_count):
    slots, columns, piece = coefs.shape
    chunks = slots // GROUP
    half_rows, lanes = legendre.shape[1:]
    quarters = half_rows // (2 * piece)
    width = 2 * lanes
    lats = width // band_count
    any_space = pl.BlockSpec(memory_space=pl.ANY)
    dma = pltpu.SemaphoreType.DMA
    shape = lambda *dims: jax.ShapeDtypeStruct(dims, jnp.float32)
    late = LATS * GROUP
    return pl.pallas_call(
        analysis_kernel,
        in_specs=[pl.BlockSpec(memory_space=pltpu.SMEM)] + [any_space] * 6,
        out_specs=[any_space] * 7,
        out_shape=[
            shape(lats * PART, NLON),
            shape(2 * TLEV, lats, NLON),
            shape(2 * TLEV, EDGE, NLON),
            shape(2 * TLEV, EDGE, NLON),
            shape(*below.shape),
            shape(*above.shape),
            shape(band_count, chunks, lats * GROUP, 2 * columns),
        ],
        scratch_shapes=[
            pltpu.VMEM((quarters, slots, columns, piece), jnp.float32),
            pltpu.VMEM((RING, half_rows, lanes), jnp.float32),
            pltpu.VMEM((chunks, width * GROUP, 2 * columns), jnp.float32),
            pltpu.VMEM(high.shape, high.dtype),
            pltpu.VMEM(low.shape, low.dtype),
            pltpu.VMEM((2, band_count, chunks, late, 2 * columns), jnp.float32),
            pltpu.VMEM((2, LATS * PART, high.shape[1]), jnp.float32),
            pltpu.VMEM((2, LATS * PART, NLON), jnp.float32),
            pltpu.VMEM((2 * TLEV, lats, NLON), jnp.float32),
            dma((RING,)),
        ]
        + [dma((chunks,))] * 7
        + [dma((2,))] * 8
        + [dma(())]
        + [dma((2,))] * 2,
        compiler_params=pltpu.CompilerParams(
            collective_id=0, has_side_effects=True, vmem_limit_bytes=63 * 1024 * 1024
        ),
    )(pairs, coefs, legendre, high, low, above, below)


def synthesis_kernel(
    pair_ref, quad_ref, heat_ref, field_ref, high_ref, low_ref, legendre_ref,
    out_ref, fourier_ref,
    bands, held, near_held, far_held, load_sem, send_sem, recv_sem, keep_sem,
    near_send, near_recv, far_send, far_recv, out_sem, table_sem, field_sem, turn_sem,
):
    slots, columns, piece = out_ref.shape
    chunks = slots // GROUP
    units = slots // UNIT
    count = lax.axis_size("ma")
    here = lax.axis_index("ma")
    quarters = lax.axis_size("pb")
    quarter = lax.axis_index("pb")
    near, far = partner(quarter, quarters, 1), partner(quarter, quarters, 2)
    band = bands.shape[1] // count
    width = bands.shape[1] // GROUP
    first_rows = LATS * GROUP
    groups = band // first_rows

    def remote(source, target, sends, receives, device):
        return pltpu.make_async_remote_copy(
            source, target, sends, receives, device_id=device, device_id_type=MESH
        )

    def send_orders(chunk, start, size):
        for step in range(1, count):
            target = (here + step) % count
            remote(
                fourier_ref.at[target, chunk, pl.ds(start, size)],
                bands.at[chunk, pl.ds(here * band + start, size)],
                send_sem, recv_sem.at[chunk], {"ma": target},
            ).start()
        pltpu.make_async_copy(
            fourier_ref.at[here, chunk, pl.ds(start, size)],
            bands.at[chunk, pl.ds(here * band + start, size)],
            keep_sem.at[chunk],
        ).start()

    for slot in range(RING - 1):
        stream_rows(legendre_ref, held, load_sem, slot).start()

    def turn(high, low, field, left, turned, block):
        tables = [
            pltpu.make_async_copy(high_ref, high, table_sem.at[0]),
            pltpu.make_async_copy(low_ref, low, table_sem.at[1]),
        ]

        def load(group):
            return pltpu.make_async_copy(
                field_ref.at[pl.ds(group * LATS * PART, LATS * PART)], field.at[group % 2],
                field_sem.at[group % 2],
            )

        def store(group):
            return pltpu.make_async_copy(
                block.at[group % 2],
                fourier_ref.at[:, :, pl.ds(group * first_rows, first_rows)],
                turn_sem.at[group % 2],
            )

        load(0).start()
        for copy in tables:
            copy.start()
        enter(count, here, quarters, quarter, [])
        for copy in tables:
            copy.wait()

        def one_group(group, carry):
            load(group).wait()

            @pl.when(group + 1 < groups)
            def _():
                load(group + 1).start()

            @pl.when(group >= 3)
            def _():
                store(group - 2).wait()

            from_grid(
                field.at[group % 2], heat_ref, pl.multiple_of(group * LATS, LATS), high, low,
                block.at[group % 2], left, turned,
            )
            store(group).start()

            @pl.when(group == 0)
            def _():
                store(group).wait()

                def first(chunk, inner):
                    send_orders(chunk, 0, first_rows)
                    return inner

                lax.fori_loop(0, chunks, first, 0)

            return carry

        lax.fori_loop(0, groups, one_group, 0)
        for group in range(max(groups - 2, 1), groups):
            store(group).wait()

    pl.run_scoped(
        turn,
        pltpu.VMEM(high_ref.shape, high_ref.dtype),
        pltpu.VMEM(low_ref.shape, low_ref.dtype),
        pltpu.VMEM((2, LATS * PART, NLON), jnp.float32),
        pltpu.VMEM((2, LATS * PART, NLON // 2), jnp.float32),
        pltpu.VMEM((LATS, 4 * PART, count * slots), jnp.float32),
        pltpu.VMEM((2, count, chunks, first_rows, 4 * PART), jnp.float32),
    )

    def rest(chunk, carry):
        send_orders(chunk, first_rows, band - first_rows)
        return carry

    if groups > 1:
        lax.fori_loop(0, chunks, rest, 0)

    def sum_up(parts):
        def to_near(unit, k):
            return remote(
                parts.at[unit, 2 * k + 1], near_held.at[unit, k],
                near_send.at[k, unit], near_recv.at[k, unit], {"pb": near},
            )

        def to_far(unit):
            return remote(
                parts.at[unit, 2], far_held.at[unit], far_send.at[unit], far_recv.at[unit],
                {"pb": far},
            )

        def store(unit):
            return pltpu.make_async_copy(
                parts.at[unit, 0], out_ref.at[pl.ds(unit * UNIT, UNIT)], out_sem.at[unit]
            )

        def one_slot(slot, unit, own):
            stream_rows(legendre_ref, held, load_sem, slot).wait()

            @pl.when(slot + RING - 1 < slots)
            def _():
                stream_rows(legendre_ref, held, load_sem, slot + RING - 1).start()

            rows = held.at[slot % RING]
            weighted = bands[slot // GROUP, pl.ds(slot % GROUP, width, GROUP), :].T * quad_ref[...]
            for k in range(quarters):
                first = (quarter if k == 0 else partner(quarter, quarters, k)) * piece
                even, odd, _ = order_rows(pair_ref, slot, first, piece)
                both = product(weighted, rows_of(rows, first, piece), (1, 1))
                parts[unit, k, own] = jnp.where(
                    even, both[:columns], jnp.where(odd, both[columns:], 0.0)
                )

        def advance(unit):
            to_near(unit, 1).wait_recv()
            for i in range(UNIT):
                parts[unit, 2, i] = parts[unit, 2, i] + near_held[unit, 1, i]
            to_far(unit).start()

        def complete(unit):
            to_near(unit, 0).wait_recv()
            to_far(unit).wait_recv()
            for i in range(UNIT):
                parts[unit, 0, i] = (
                    parts[unit, 0, i] + near_held[unit, 0, i] + far_held[unit, i]
                )
            store(unit).start()

        lag = 2 * (GROUP // UNIT)

        def one_unit(unit, carry):
            @pl.when(unit % (GROUP // UNIT) == 0)
            def _():
                chunk = unit // (GROUP // UNIT)
                wait_bytes(bands.at[chunk, pl.ds(0, band)], keep_sem.at[chunk])
                wait_bytes(bands.at[chunk, pl.ds(0, (count - 1) * band)], recv_sem.at[chunk])

            def body(i, inner):
                one_slot(unit * UNIT + i, unit, i)
                return inner

            lax.fori_loop(0, UNIT, body, 0)
            to_near(unit, 1).start()
            to_near(unit, 0).start()

            @pl.when(unit > 0)
            def _():
                advance(unit - 1)

            @pl.when(unit >= lag)
            def _():
                complete(unit - lag)

            return carry

        lax.fori_loop(0, units, one_unit, 0)
        advance(units - 1)

        def last(i, carry):
            complete(units - lag + i)
            return carry

        lax.fori_loop(0, lag, last, 0)

        def finish(unit, carry):
            to_near(unit, 0).wait_send()
            to_near(unit, 1).wait_send()
            to_far(unit).wait_send()
            store(unit).wait()
            return carry

        lax.fori_loop(0, units, finish, 0)
        wait_bytes(fourier_ref.at[pl.ds(0, count - 1)], send_sem)

    pl.run_scoped(sum_up, pltpu.VMEM((units, quarters, UNIT, columns, piece), jnp.float32))


def synthesis(pairs, quad, heat, field, high, low, legendre, piece, band_count):
    slots = pairs.shape[0]
    chunks = slots // GROUP
    units = slots // UNIT
    lats = heat.shape[1]
    columns = 2 * PART
    half_rows, lanes = legendre.shape[1:]
    any_space = pl.BlockSpec(memory_space=pl.ANY)
    vmem = pl.BlockSpec(memory_space=pltpu.VMEM)
    dma = pltpu.SemaphoreType.DMA
    block = (UNIT, columns, piece)
    return pl.pallas_call(
        synthesis_kernel,
        in_specs=[pl.BlockSpec(memory_space=pltpu.SMEM), vmem, vmem] + [any_space] * 4,
        out_specs=[any_space] * 2,
        out_shape=[
            jax.ShapeDtypeStruct((slots, columns, piece), jnp.float32),
            jax.ShapeDtypeStruct((band_count, chunks, lats * GROUP, 2 * columns), jnp.float32),
        ],
        scratch_shapes=[
            pltpu.VMEM((chunks, band_count * lats * GROUP, 2 * columns), jnp.float32),
            pltpu.VMEM((RING, half_rows, lanes), jnp.float32),
            pltpu.VMEM((units, 2) + block, jnp.float32),
            pltpu.VMEM((units,) + block, jnp.float32),
            dma((RING,)),
            dma(()),
            dma((chunks,)),
            dma((chunks,)),
            dma((2, units)),
            dma((2, units)),
            dma((units,)),
            dma((units,)),
            dma((units,)),
            dma((2,)),
            dma((2,)),
            dma((2,)),
        ],
        compiler_params=pltpu.CompilerParams(
            collective_id=1, has_side_effects=True, vmem_limit_bytes=63 * 1024 * 1024
        ),
    )(pairs, quad, heat, field, high, low, legendre)[0]


def shards(coefs, legendre, quad_weight, pair_of_slot, tracers, heat_rate):
    slot_count, piece = coefs.shape[:2]
    quarter = legendre.shape[3]
    band_count = lax.axis_size("ma")
    band_rows = tracers.shape[2]
    lanes = 128
    legendre_rows = legendre.reshape(slot_count, -1, lanes)
    own_pairs = lax.dynamic_slice_in_dim(
        pair_of_slot, lax.axis_index("ma") * slot_count, slot_count, 0
    )
    table_high, table_low = fourier_tables(pair_of_slot)
    field, wind, wind_low, wind_high, low, high, _ = analysis(
        own_pairs, jnp.transpose(coefs, (0, 2, 1)), legendre_rows, table_high, table_low,
        tracers[:, :, :HALO], tracers[:, :, band_rows - HALO :], band_count,
    )
    first_row = (lax.axis_index(("ma", "pb")) * band_rows).astype(jnp.int32)
    new_tracers, heating = transport(
        first_row, heat_rate, tracers, low, high, wind, wind_low, wind_high
    )
    spec = synthesis(
        own_pairs, quad_weight.reshape(1, quarter), heating, field, table_high, table_low,
        legendre_rows, piece, band_count,
    )
    return (jnp.transpose(spec, (0, 2, 1)), new_tracers)


def solution(mesh):
    in_specs = (
        P("ma", "pb", None),
        P("ma", None, "pb", None),
        P("pb", None),
        P(),
        P(None, None, ("ma", "pb"), None),
        P(),
    )
    out_specs = (P("ma", "pb", None), P(None, None, ("ma", "pb"), None))
    return jax.shard_map(shards, mesh=mesh, in_specs=in_specs, out_specs=out_specs, check_vma=False)
```

```python
import math

import jax
import jax.numpy as jnp
from jax import lax
from jax.experimental import pallas as pl
from jax.experimental.pallas import tpu as pltpu
from jax.sharding import PartitionSpec as P

M = 1024
NLAT = 1024
NLON = 2048
LAYER_TOTAL = 8
NF = 4
NTR = 12
TLEV = 2
PAIRS = 512


COURANT = 0.15
DRAG_COEFFICIENT = 0.2
MOISTURE_SOURCE = 0.3
RAINFALL_FACTOR = 0.2
HIGH = lax.Precision.HIGH

HALO = 3
EDGE = 8


def split_orders(pair_ids):
    low_even = pair_ids % 2 == 0
    even = jnp.where(low_even, pair_ids, M - 1 - pair_ids)
    return low_even, even, M - 1 - even


def half_tables(orders, points):
    step = 128
    coarse_ids = jnp.arange(points // step, dtype=jnp.int32) * step
    fine_ids = jnp.arange(step, dtype=jnp.int32)
    unit = 2.0 * math.pi / NLON
    coarse = (orders[:, None] * coarse_ids[None, :] % NLON).astype(jnp.float32) * unit
    fine = (orders[:, None] * fine_ids[None, :] % NLON).astype(jnp.float32) * unit
    factor = 1.0 / math.sqrt(NLON)
    cc, sc = lax.optimization_barrier((jnp.cos(coarse) * factor, jnp.sin(coarse) * factor))
    cf, sf = lax.optimization_barrier((jnp.cos(fine), jnp.sin(fine)))
    cos = [cc[:, a : a + 1] * cf - sc[:, a : a + 1] * sf for a in range(points // step)]
    sin = [-(sc[:, a : a + 1] * cf + cc[:, a : a + 1] * sf) for a in range(points // step)]
    return jnp.stack([jnp.concatenate(cos, axis=1), jnp.concatenate(sin, axis=1)], axis=0)


MESH = pl.DeviceIdType.MESH
GROUP = 8
RING = 4
LATS = 8
UNIT = 2
PART = NF * LAYER_TOTAL


def partner(index, count, step):
    if step == 1:
        return index + 1 - 2 * (index % 2)
    if step == 2:
        return (index + count // 2) % count
    return count - 1 - index


def split(x):
    high = x.astype(jnp.bfloat16)
    return high, (x - high.astype(jnp.float32)).astype(jnp.bfloat16)


def product(left, right, contract):
    dims = ((contract[:1], contract[1:]), ((), ()))
    rows = left.shape[0]
    left_high, left_low = split(left)
    right_high, right_low = split(right)
    both = lax.dot_general(
        jnp.concatenate([left_high, left_low], axis=0), right_high, dims,
        preferred_element_type=jnp.float32,
    )
    rest = lax.dot_general(left_high, right_low, dims, preferred_element_type=jnp.float32)
    return both[:rows] + (both[rows:] + rest)


def rows_of(ref, start, count):
    return jnp.concatenate(
        [ref[pl.ds(2 * start, count, 2), :], ref[pl.ds(2 * start + 1, count, 2), :]], axis=1
    )


def order_rows(pair_ref, slot, first, count):
    pair = pair_ref[slot]
    bound = M - pair
    low_even = pair % 2 == 0
    even_from, even_to = jnp.where(low_even, 0, bound), jnp.where(low_even, bound, M + 1)
    odd_from, odd_to = jnp.where(low_even, bound, 0), jnp.where(low_even, M + 1, bound)
    rows = first + lax.broadcasted_iota(jnp.int32, (1, count), 1)
    even = (rows >= even_from) & (rows < even_to)
    odd = (rows >= odd_from) & (rows < odd_to)
    return even, odd, jnp.where(pair == 0, 1.0, 2.0)


def fourier_tables(pair_of_slot):
    _, even_all, odd_all = split_orders(pair_of_slot)
    half = NLON // 2
    tables = jnp.stack([half_tables(even_all, half), half_tables(odd_all, half)], axis=0)
    tables = tables.reshape(2, -1, half)
    high = lax.reduce_precision(tables, 8, 7)
    return high.astype(jnp.bfloat16), (tables - high).astype(jnp.bfloat16)


def transport_kernel(
    first_ref, rate_ref, q_ref, ql_ref, qh_ref, u_ref, ul_ref, uh_ref, w_ref, wl_ref, wh_ref,
    out_ref, heat_ref, pad, ap, an, bp, bn,
):
    rows = q_ref.shape[2]
    total = rows + EDGE
    lons = q_ref.shape[3]
    level = pl.program_id(0)
    tracer = pl.program_id(1)
    edge_rows = lax.broadcasted_iota(jnp.int32, (EDGE, lons), 0)

    @pl.when(tracer == 0)
    def _():
        pad[0:EDGE, :] = jnp.where(edge_rows < EDGE // 2, uh_ref[0], ul_ref[0])
        pad[EDGE:total, :] = u_ref[0]
        u = pad[...]
        face = (0.5 * COURANT) * (u + pltpu.roll(u, lons - 1, 1))
        ap[...] = jnp.maximum(face, 0.0)
        an[...] = jnp.minimum(face, 0.0)
        pad[0:EDGE, :] = jnp.where(edge_rows < EDGE // 2, wh_ref[0], wl_ref[0])
        pad[EDGE:total, :] = w_ref[0]
        w = pad[...]
        face = (-0.5 * COURANT) * (w + pltpu.roll(w, total - 1, 0))
        place = lax.broadcasted_iota(jnp.int32, (total, lons), 0)
        upper = first_ref[0] + jnp.where(place < EDGE // 2, rows + place, place - EDGE)
        inside = (upper >= 0) & (upper <= NLAT - 2)
        bp[...] = jnp.where(inside, jnp.maximum(face, 0.0), 0.0)
        bn[...] = jnp.where(inside, jnp.minimum(face, 0.0), 0.0)
        pad[0:EDGE, :] = jnp.zeros((EDGE, lons), jnp.float32)

    def step(q):
        east = ap[...] * q + an[...] * pltpu.roll(q, lons - 1, 1)
        south = bp[...] * q + bn[...] * pltpu.roll(q, total - 1, 0)
        return q - ((east - pltpu.roll(east, 1, 1)) + (south - pltpu.roll(south, 1, 0)))

    pad[0:HALO, :] = qh_ref[0, 0]
    pad[EDGE - HALO : EDGE, :] = ql_ref[0, 0]
    pad[EDGE:total, :] = q_ref[0, 0]
    q = pad[...]
    second = 0.75 * q + 0.25 * step(step(q))
    third = step(second)[EDGE:total]
    new = q_ref[0, 0] * (1.0 / 3.0) + (2.0 / 3.0) * third
    out_ref[0, 0] = new
    warm = rate_ref[tracer, level] * new

    @pl.when(tracer == 0)
    def _():
        heat_ref[0] = warm

    @pl.when(tracer > 0)
    def _():
        heat_ref[0] += warm


def transport(first_row, heat_rate, tracers, low, high, wind, wind_low, wind_high):
    count, levels, rows, lons = tracers.shape
    total = rows + EDGE

    def tracer_spec(height):
        return pl.BlockSpec((1, 1, height, lons), lambda l, k: (k, l, 0, 0))

    def wind_spec(height, first):
        return pl.BlockSpec((1, height, lons), lambda l, k: (l + first, 0, 0))

    smem = pl.BlockSpec(memory_space=pltpu.SMEM)
    return pl.pallas_call(
        transport_kernel,
        grid=(levels, count),
        in_specs=[smem, smem]
        + [tracer_spec(rows), tracer_spec(HALO), tracer_spec(HALO)]
        + [wind_spec(rows, 0), wind_spec(EDGE, 0), wind_spec(EDGE, 0)]
        + [wind_spec(rows, levels), wind_spec(EDGE, levels), wind_spec(EDGE, levels)],
        out_specs=[tracer_spec(rows), wind_spec(rows, 0)],
        out_shape=[
            jax.ShapeDtypeStruct(tracers.shape, tracers.dtype),
            jax.ShapeDtypeStruct((levels, rows, lons), tracers.dtype),
        ],
        scratch_shapes=[pltpu.VMEM((total, lons), jnp.float32)] * 5,
        compiler_params=pltpu.CompilerParams(
            dimension_semantics=("arbitrary", "arbitrary"), vmem_limit_bytes=63 * 1024 * 1024
        ),
    )(
        first_row.reshape(1), heat_rate, tracers, low, high,
        wind, wind_low, wind_high, wind, wind_low, wind_high,
    )


def neighbour(band, count, quarter, quarters, step):
    place = (band * quarters + quarter + step + count * quarters) % (count * quarters)
    return {"ma": place // quarters, "pb": place % quarters}


def enter(band_count, here, quarter_count, quarter, beside):
    barrier = pltpu.get_barrier_semaphore()
    others = [{"ma": (here + step) % band_count} for step in range(1, band_count)]
    others += [{"pb": partner(quarter, quarter_count, step)} for step in (1, 2)]
    for other in others + beside:
        pl.semaphore_signal(barrier, inc=1, device_id=other, device_id_type=MESH)
    pl.semaphore_wait(barrier, len(others) + len(beside))


def stream_rows(legendre_ref, held, sem, slot):
    return pltpu.make_async_copy(legendre_ref.at[slot], held.at[slot % RING], sem.at[slot % RING])


def wait_bytes(ref, sem):
    pltpu.make_async_copy(ref, ref, sem).wait()


def to_grid(spectral_ref, high_ref, low_ref, out_ref, left):
    sources, chunks = spectral_ref.shape[:2]
    slots = sources * chunks * GROUP
    half = high_ref.shape[2]
    for j in range(LATS):
        block = spectral_ref[:, :, j * GROUP : (j + 1) * GROUP, :].reshape(slots, 4 * PART).T
        for h in range(2):
            for p in range(2):
                left[h, j * PART : (j + 1) * PART, p * slots : (p + 1) * slots] = block[
                    (2 * h + p) * PART : (2 * h + p + 1) * PART
                ]
    sums = []
    for h in range(2):
        high, low = split(left[h])
        dot = lambda a, b: jnp.dot(a, b, preferred_element_type=jnp.float32)
        sums.append(dot(high, high_ref[h]) + (dot(low, high_ref[h]) + dot(high, low_ref[h])))
    out_ref[:, :half] = sums[0] + sums[1]
    out_ref[:, half:] = sums[0] - sums[1]


def from_grid(field_ref, heat_ref, first, high_ref, low_ref, out_ref, left, turned):
    sources, chunks = out_ref.shape[:2]
    slots = sources * chunks * GROUP
    half = high_ref.shape[2]
    lev = LAYER_TOTAL
    level = lax.broadcasted_iota(jnp.int32, (lev, half), 0)

    for j in range(LATS):
        def tendency(start):
            cols = slice(start, start + half)
            at = lambda f: field_ref[j * PART + f * lev : j * PART + (f + 1) * lev, cols]
            u, v, t, q = at(0), at(1), at(2), at(3)
            speed = jnp.sqrt(u * u + v * v + 1.0)
            moist = MOISTURE_SOURCE * t * q
            warm = jnp.zeros((lev, half), jnp.float32)
            for l in range(TLEV):
                rows = heat_ref[l, pl.ds(first, LATS), cols]
                warm = jnp.where(level == l, rows[j : j + 1], warm)
            return jnp.concatenate(
                [
                    -DRAG_COEFFICIENT * speed * u,
                    -DRAG_COEFFICIENT * speed * v,
                    warm - moist,
                    moist - RAINFALL_FACTOR * speed * q,
                ],
                axis=0,
            )

        near = tendency(0)
        far = tendency(half)
        left[0, j * PART : (j + 1) * PART] = near + far
        left[1, j * PART : (j + 1) * PART] = near - far
    dims = (((1,), (1,)), ((), ()))
    for h in range(2):
        high, low = split(left[h])
        dot = lambda a, b: lax.dot_general(a, b, dims, preferred_element_type=jnp.float32)
        both = dot(high, high_ref[h]) + (dot(low, high_ref[h]) + dot(high, low_ref[h]))
        for j in range(LATS):
            for p in range(2):
                turned[j, (2 * h + p) * PART : (2 * h + p + 1) * PART] = both[
                    j * PART : (j + 1) * PART, p * slots : (p + 1) * slots
                ]
    for j in range(LATS):
        out_ref[:, :, j * GROUP : (j + 1) * GROUP, :] = turned[j].T.reshape(
            sources, chunks, GROUP, 4 * PART
        )


def analysis_kernel(
    pair_ref, coefs_ref, legendre_ref, high_ref, low_ref, above_ref, below_ref,
    field_ref, wind_ref, wind_low_ref, wind_high_ref, trace_low_ref, trace_high_ref, bands_ref,
    pieces, held, sums, high, low, block, left, field, wind,
    load_sem, own_sem, near_send, near_recv, far_send, far_recv,
    pass_send, pass_recv, send_sem, recv_sem, keep_sem, table_sem, trace_send, trace_recv,
    block_sem, field_sem, wind_sem, edge_send, edge_recv,
):
    slots, columns, piece = coefs_ref.shape
    chunks = slots // GROUP
    count = lax.axis_size("ma")
    here = lax.axis_index("ma")
    quarters = lax.axis_size("pb")
    quarter = lax.axis_index("pb")
    near, far = partner(quarter, quarters, 1), partner(quarter, quarters, 2)
    after = neighbour(here, count, quarter, quarters, 1)
    before = neighbour(here, count, quarter, quarters, -1)
    band = sums.shape[1] // count
    width = sums.shape[1] // GROUP
    weight_columns = 2 * columns
    groups = band // (LATS * GROUP)
    late = LATS * GROUP
    early = band - late
    spans = ((0, early), (early, late))

    def part(ref, chunk):
        return ref.at[pl.ds(chunk * GROUP, GROUP)]

    def remote(source, target, sends, receives, device):
        return pltpu.make_async_remote_copy(
            source, target, sends, receives, device_id=device, device_id_type=MESH
        )

    def own(chunk):
        return pltpu.make_async_copy(
            part(coefs_ref, chunk), part(pieces.at[0], chunk), own_sem.at[chunk]
        )

    def to_near(chunk):
        return remote(
            part(coefs_ref, chunk), part(pieces.at[1], chunk),
            near_send.at[chunk], near_recv.at[chunk], {"pb": near},
        )

    def to_far(chunk):
        return remote(
            part(coefs_ref, chunk), part(pieces.at[2], chunk),
            far_send.at[chunk], far_recv.at[chunk], {"pb": far},
        )

    def pass_on(chunk):
        return remote(
            part(pieces.at[2], chunk), part(pieces.at[3], chunk),
            pass_send.at[chunk], pass_recv.at[chunk], {"pb": near},
        )

    def send_bands(chunk, which):
        start, size = spans[which]
        for step in range(1, count):
            target = (here + step) % count
            remote(
                sums.at[chunk, pl.ds(target * band + start, size)],
                bands_ref.at[here, chunk, pl.ds(start, size)],
                send_sem.at[which], recv_sem.at[which], {"ma": target},
            ).start()
        pltpu.make_async_copy(
            sums.at[chunk, pl.ds(here * band + start, size)],
            bands_ref.at[here, chunk, pl.ds(start, size)],
            keep_sem.at[which],
        ).start()

    def wait_bands(which):
        start, size = spans[which]
        wait_bytes(bands_ref.at[pl.ds(0, count - 1), :, pl.ds(start, size)], recv_sem.at[which])
        wait_bytes(bands_ref.at[0, :, pl.ds(start, size)], keep_sem.at[which])

    tables = [
        pltpu.make_async_copy(high_ref, high, table_sem.at[0]),
        pltpu.make_async_copy(low_ref, low, table_sem.at[1]),
    ]
    traces = [
        remote(above_ref, trace_high_ref, trace_send.at[0], trace_recv.at[0], before),
        remote(below_ref, trace_low_ref, trace_send.at[1], trace_recv.at[1], after),
    ]

    for slot in range(RING - 1):
        stream_rows(legendre_ref, held, load_sem, slot).start()
    enter(count, here, quarters, quarter, [after, before])

    def begin(chunk, carry):
        to_far(chunk).start()
        to_near(chunk).start()
        own(chunk).start()
        return carry

    lax.fori_loop(0, chunks, begin, 0)

    def one_slot(slot, chunk):
        stream_rows(legendre_ref, held, load_sem, slot).wait()

        @pl.when(slot + RING - 1 < slots)
        def _():
            stream_rows(legendre_ref, held, load_sem, slot + RING - 1).start()

        rows = held.at[slot % RING]
        total = jnp.zeros((weight_columns, width), jnp.float32)
        main = piece - piece % 128
        ends, end_rows = [], []
        for k in range(quarters):
            first = (quarter if k == 0 else partner(quarter, quarters, k)) * piece
            even, odd, even_weight = order_rows(pair_ref, slot, first, piece)
            x = pieces[k, slot]
            both = jnp.concatenate(
                [jnp.where(even, x * even_weight, 0.0), jnp.where(odd, x * 2.0, 0.0)], axis=0
            )
            total = total + product(both[:, :main], rows_of(rows, first, main), (1, 0))
            ends.append(both[:, main:])
            end_rows.append(rows_of(rows, first + main, piece - main))
        total = total + product(
            jnp.concatenate(ends, axis=1), jnp.concatenate(end_rows, axis=0), (1, 0)
        )
        sums[chunk, pl.ds(slot % GROUP, width, GROUP), :] = total.T

    def one_chunk(chunk, carry):
        to_far(chunk).wait_recv()
        pass_on(chunk).start()
        own(chunk).wait()
        to_near(chunk).wait_recv()
        pass_on(chunk).wait_recv()

        def body(i, inner):
            one_slot(chunk * GROUP + i, chunk)
            return inner

        lax.fori_loop(0, GROUP, body, 0)
        if early:
            send_bands(chunk, 0)
        return carry

    lax.fori_loop(0, chunks, one_chunk, 0)

    def send_late(chunk, carry):
        send_bands(chunk, 1)
        return carry

    lax.fori_loop(0, chunks, send_late, 0)
    for copy in tables + traces:
        copy.start()

    def load(group):
        return pltpu.make_async_copy(
            bands_ref.at[:, :, pl.ds(group * late, late)], block.at[group % 2],
            block_sem.at[group % 2],
        )

    def store(group):
        return pltpu.make_async_copy(
            field.at[group % 2], field_ref.at[pl.ds(group * LATS * PART, LATS * PART)],
            field_sem.at[group % 2],
        )

    for copy in tables:
        copy.wait()
    wait_bands(0 if early else 1)
    load(0).start()

    def one_group(group, carry):
        load(group).wait()

        @pl.when(group + 2 < groups)
        def _():
            load(group + 1).start()

        @pl.when(group + 2 == groups)
        def _():
            wait_bands(1)
            load(group + 1).start()

        @pl.when(group >= 2)
        def _():
            store(group - 2).wait()

        to_grid(block.at[group % 2], high, low, field.at[group % 2], left)
        store(group).start()
        for component in range(2):
            for l in range(TLEV):
                row = component * LAYER_TOTAL + l
                wind[component * TLEV + l, pl.ds(group * LATS, LATS), :] = jnp.concatenate(
                    [
                        field[group % 2, j * PART + row : j * PART + row + 1, :]
                        for j in range(LATS)
                    ],
                    axis=0,
                )
        return carry

    lax.fori_loop(0, groups, one_group, 0)
    lats = groups * LATS
    edges = [
        remote(
            wind.at[:, pl.ds(0, EDGE)], wind_high_ref, edge_send.at[0], edge_recv.at[0], before
        ),
        remote(
            wind.at[:, pl.ds(lats - EDGE, EDGE)], wind_low_ref,
            edge_send.at[1], edge_recv.at[1], after,
        ),
    ]
    winds = pltpu.make_async_copy(wind, wind_ref, wind_sem)
    for copy in edges + [winds]:
        copy.start()

    def finish(chunk, carry):
        to_far(chunk).wait_send()
        to_near(chunk).wait_send()
        pass_on(chunk).wait_send()
        return carry

    lax.fori_loop(0, chunks, finish, 0)
    for which in range(0 if early else 1, 2):
        start, size = spans[which]
        wait_bytes(bands_ref.at[pl.ds(0, count - 1), :, pl.ds(start, size)], send_sem.at[which])
    for group in range(max(groups - 2, 0), groups):
        store(group).wait()
    for copy in traces + edges + [winds]:
        copy.wait()


def analysis(pairs, coefs, legendre, high, low, above, below, band_count):
    slots, columns, piece = coefs.shape
    chunks = slots // GROUP
    half_rows, lanes = legendre.shape[1:]
    quarters = half_rows // (2 * piece)
    width = 2 * lanes
    lats = width // band_count
    any_space = pl.BlockSpec(memory_space=pl.ANY)
    dma = pltpu.SemaphoreType.DMA
    shape = lambda *dims: jax.ShapeDtypeStruct(dims, jnp.float32)
    late = LATS * GROUP
    return pl.pallas_call(
        analysis_kernel,
        in_specs=[pl.BlockSpec(memory_space=pltpu.SMEM)] + [any_space] * 6,
        out_specs=[any_space] * 7,
        out_shape=[
            shape(lats * PART, NLON),
            shape(2 * TLEV, lats, NLON),
            shape(2 * TLEV, EDGE, NLON),
            shape(2 * TLEV, EDGE, NLON),
            shape(*below.shape),
            shape(*above.shape),
            shape(band_count, chunks, lats * GROUP, 2 * columns),
        ],
        scratch_shapes=[
            pltpu.VMEM((quarters, slots, columns, piece), jnp.float32),
            pltpu.VMEM((RING, half_rows, lanes), jnp.float32),
            pltpu.VMEM((chunks, width * GROUP, 2 * columns), jnp.float32),
            pltpu.VMEM(high.shape, high.dtype),
            pltpu.VMEM(low.shape, low.dtype),
            pltpu.VMEM((2, band_count, chunks, late, 2 * columns), jnp.float32),
            pltpu.VMEM((2, LATS * PART, high.shape[1]), jnp.float32),
            pltpu.VMEM((2, LATS * PART, NLON), jnp.float32),
            pltpu.VMEM((2 * TLEV, lats, NLON), jnp.float32),
            dma((RING,)),
        ]
        + [dma((chunks,))] * 7
        + [dma((2,))] * 8
        + [dma(())]
        + [dma((2,))] * 2,
        compiler_params=pltpu.CompilerParams(
            collective_id=0, has_side_effects=True, vmem_limit_bytes=63 * 1024 * 1024
        ),
    )(pairs, coefs, legendre, high, low, above, below)


def synthesis_kernel(
    pair_ref, quad_ref, heat_ref, field_ref, high_ref, low_ref, legendre_ref,
    out_ref, fourier_ref,
    bands, held, near_held, far_held, load_sem, send_sem, recv_sem, keep_sem,
    near_send, near_recv, far_send, far_recv, out_sem, table_sem, field_sem, turn_sem,
):
    slots, columns, piece = out_ref.shape
    chunks = slots // GROUP
    units = slots // UNIT
    count = lax.axis_size("ma")
    here = lax.axis_index("ma")
    quarters = lax.axis_size("pb")
    quarter = lax.axis_index("pb")
    near, far = partner(quarter, quarters, 1), partner(quarter, quarters, 2)
    band = bands.shape[1] // count
    width = bands.shape[1] // GROUP
    first_rows = LATS * GROUP
    groups = band // first_rows

    def remote(source, target, sends, receives, device):
        return pltpu.make_async_remote_copy(
            source, target, sends, receives, device_id=device, device_id_type=MESH
        )

    def send_orders(chunk, start, size):
        for step in range(1, count):
            target = (here + step) % count
            remote(
                fourier_ref.at[target, chunk, pl.ds(start, size)],
                bands.at[chunk, pl.ds(here * band + start, size)],
                send_sem, recv_sem.at[chunk], {"ma": target},
            ).start()
        pltpu.make_async_copy(
            fourier_ref.at[here, chunk, pl.ds(start, size)],
            bands.at[chunk, pl.ds(here * band + start, size)],
            keep_sem.at[chunk],
        ).start()

    for slot in range(RING - 1):
        stream_rows(legendre_ref, held, load_sem, slot).start()

    def turn(high, low, field, left, turned, block):
        tables = [
            pltpu.make_async_copy(high_ref, high, table_sem.at[0]),
            pltpu.make_async_copy(low_ref, low, table_sem.at[1]),
        ]

        def load(group):
            return pltpu.make_async_copy(
                field_ref.at[pl.ds(group * LATS * PART, LATS * PART)], field.at[group % 2],
                field_sem.at[group % 2],
            )

        def store(group):
            return pltpu.make_async_copy(
                block.at[group % 2],
                fourier_ref.at[:, :, pl.ds(group * first_rows, first_rows)],
                turn_sem.at[group % 2],
            )

        load(0).start()
        for copy in tables:
            copy.start()
        enter(count, here, quarters, quarter, [])
        for copy in tables:
            copy.wait()

        def one_group(group, carry):
            load(group).wait()

            @pl.when(group + 1 < groups)
            def _():
                load(group + 1).start()

            @pl.when(group >= 3)
            def _():
                store(group - 2).wait()

            from_grid(
                field.at[group % 2], heat_ref, pl.multiple_of(group * LATS, LATS), high, low,
                block.at[group % 2], left, turned,
            )
            store(group).start()

            @pl.when(group == 0)
            def _():
                store(group).wait()

                def first(chunk, inner):
                    send_orders(chunk, 0, first_rows)
                    return inner

                lax.fori_loop(0, chunks, first, 0)

            return carry

        lax.fori_loop(0, groups, one_group, 0)
        for group in range(max(groups - 2, 1), groups):
            store(group).wait()

    pl.run_scoped(
        turn,
        pltpu.VMEM(high_ref.shape, high_ref.dtype),
        pltpu.VMEM(low_ref.shape, low_ref.dtype),
        pltpu.VMEM((2, LATS * PART, NLON), jnp.float32),
        pltpu.VMEM((2, LATS * PART, NLON // 2), jnp.float32),
        pltpu.VMEM((LATS, 4 * PART, count * slots), jnp.float32),
        pltpu.VMEM((2, count, chunks, first_rows, 4 * PART), jnp.float32),
    )

    def rest(chunk, carry):
        send_orders(chunk, first_rows, band - first_rows)
        return carry

    if groups > 1:
        lax.fori_loop(0, chunks, rest, 0)

    def sum_up(parts):
        def to_near(unit, k):
            return remote(
                parts.at[unit, 2 * k + 1], near_held.at[unit, k],
                near_send.at[k, unit], near_recv.at[k, unit], {"pb": near},
            )

        def to_far(unit):
            return remote(
                parts.at[unit, 2], far_held.at[unit], far_send.at[unit], far_recv.at[unit],
                {"pb": far},
            )

        def store(unit):
            return pltpu.make_async_copy(
                parts.at[unit, 0], out_ref.at[pl.ds(unit * UNIT, UNIT)], out_sem.at[unit]
            )

        def one_slot(slot, unit, own):
            stream_rows(legendre_ref, held, load_sem, slot).wait()

            @pl.when(slot + RING - 1 < slots)
            def _():
                stream_rows(legendre_ref, held, load_sem, slot + RING - 1).start()

            rows = held.at[slot % RING]
            weighted = bands[slot // GROUP, pl.ds(slot % GROUP, width, GROUP), :].T * quad_ref[...]
            main = piece - piece % 128
            rest = piece - main
            firsts = [
                (quarter if k == 0 else partner(quarter, quarters, k)) * piece
                for k in range(quarters)
            ]
            ends = product(
                weighted,
                jnp.concatenate([rows_of(rows, first + main, rest) for first in firsts], axis=0),
                (1, 1),
            )
            for k, first in enumerate(firsts):
                both = product(weighted, rows_of(rows, first, main), (1, 1))
                for start, size, sums in (
                    (0, main, both), (main, rest, ends[:, k * rest : (k + 1) * rest])
                ):
                    even, odd, _ = order_rows(pair_ref, slot, first + start, size)
                    parts[unit, k, own, :, start : start + size] = jnp.where(
                        even, sums[:columns], jnp.where(odd, sums[columns:], 0.0)
                    )

        def advance(unit):
            to_near(unit, 1).wait_recv()
            for i in range(UNIT):
                parts[unit, 2, i] = parts[unit, 2, i] + near_held[unit, 1, i]
            to_far(unit).start()

        def complete(unit):
            to_near(unit, 0).wait_recv()
            to_far(unit).wait_recv()
            for i in range(UNIT):
                parts[unit, 0, i] = (
                    parts[unit, 0, i] + near_held[unit, 0, i] + far_held[unit, i]
                )
            store(unit).start()

        lag = 2 * (GROUP // UNIT)

        def one_unit(unit, carry):
            @pl.when(unit % (GROUP // UNIT) == 0)
            def _():
                chunk = unit // (GROUP // UNIT)
                wait_bytes(bands.at[chunk, pl.ds(0, band)], keep_sem.at[chunk])
                wait_bytes(bands.at[chunk, pl.ds(0, (count - 1) * band)], recv_sem.at[chunk])

            def body(i, inner):
                one_slot(unit * UNIT + i, unit, i)
                return inner

            lax.fori_loop(0, UNIT, body, 0)
            to_near(unit, 1).start()
            to_near(unit, 0).start()

            @pl.when(unit > 0)
            def _():
                advance(unit - 1)

            @pl.when(unit >= lag)
            def _():
                complete(unit - lag)

            return carry

        lax.fori_loop(0, units, one_unit, 0)
        advance(units - 1)

        def last(i, carry):
            complete(units - lag + i)
            return carry

        lax.fori_loop(0, lag, last, 0)

        def finish(unit, carry):
            to_near(unit, 0).wait_send()
            to_near(unit, 1).wait_send()
            to_far(unit).wait_send()
            store(unit).wait()
            return carry

        lax.fori_loop(0, units, finish, 0)
        wait_bytes(fourier_ref.at[pl.ds(0, count - 1)], send_sem)

    pl.run_scoped(sum_up, pltpu.VMEM((units, quarters, UNIT, columns, piece), jnp.float32))


def synthesis(pairs, quad, heat, field, high, low, legendre, piece, band_count):
    slots = pairs.shape[0]
    chunks = slots // GROUP
    units = slots // UNIT
    lats = heat.shape[1]
    columns = 2 * PART
    half_rows, lanes = legendre.shape[1:]
    any_space = pl.BlockSpec(memory_space=pl.ANY)
    vmem = pl.BlockSpec(memory_space=pltpu.VMEM)
    dma = pltpu.SemaphoreType.DMA
    block = (UNIT, columns, piece)
    return pl.pallas_call(
        synthesis_kernel,
        in_specs=[pl.BlockSpec(memory_space=pltpu.SMEM), vmem, vmem] + [any_space] * 4,
        out_specs=[any_space] * 2,
        out_shape=[
            jax.ShapeDtypeStruct((slots, columns, piece), jnp.float32),
            jax.ShapeDtypeStruct((band_count, chunks, lats * GROUP, 2 * columns), jnp.float32),
        ],
        scratch_shapes=[
            pltpu.VMEM((chunks, band_count * lats * GROUP, 2 * columns), jnp.float32),
            pltpu.VMEM((RING, half_rows, lanes), jnp.float32),
            pltpu.VMEM((units, 2) + block, jnp.float32),
            pltpu.VMEM((units,) + block, jnp.float32),
            dma((RING,)),
            dma(()),
            dma((chunks,)),
            dma((chunks,)),
            dma((2, units)),
            dma((2, units)),
            dma((units,)),
            dma((units,)),
            dma((units,)),
            dma((2,)),
            dma((2,)),
            dma((2,)),
        ],
        compiler_params=pltpu.CompilerParams(
            collective_id=1, has_side_effects=True, vmem_limit_bytes=63 * 1024 * 1024
        ),
    )(pairs, quad, heat, field, high, low, legendre)[0]


def shards(coefs, legendre, quad_weight, pair_of_slot, tracers, heat_rate):
    slot_count, piece = coefs.shape[:2]
    quarter = legendre.shape[3]
    band_count = lax.axis_size("ma")
    band_rows = tracers.shape[2]
    lanes = 128
    legendre_rows = legendre.reshape(slot_count, -1, lanes)
    own_pairs = lax.dynamic_slice_in_dim(
        pair_of_slot, lax.axis_index("ma") * slot_count, slot_count, 0
    )
    table_high, table_low = fourier_tables(pair_of_slot)
    field, wind, wind_low, wind_high, low, high, _ = analysis(
        own_pairs, jnp.transpose(coefs, (0, 2, 1)), legendre_rows, table_high, table_low,
        tracers[:, :, :HALO], tracers[:, :, band_rows - HALO :], band_count,
    )
    first_row = (lax.axis_index(("ma", "pb")) * band_rows).astype(jnp.int32)
    new_tracers, heating = transport(
        first_row, heat_rate, tracers, low, high, wind, wind_low, wind_high
    )
    spec = synthesis(
        own_pairs, quad_weight.reshape(1, quarter), heating, field, table_high, table_low,
        legendre_rows, piece, band_count,
    )
    return (jnp.transpose(spec, (0, 2, 1)), new_tracers)


def solution(mesh):
    in_specs = (
        P("ma", "pb", None),
        P("ma", None, "pb", None),
        P("pb", None),
        P(),
        P(None, None, ("ma", "pb"), None),
        P(),
    )
    out_specs = (P("ma", "pb", None), P(None, None, ("ma", "pb"), None))
    return jax.shard_map(shards, mesh=mesh, in_specs=in_specs, out_specs=out_specs, check_vma=False)
```
